128 devices in a mesh: batch: 1, g: 128 (over z, y, x, core).
Axes of the slice: x: 4, y: 4, z: 4, core: 2. Of those that a mesh axis runs over, the one named last changes fastest.
Arguments:
- keys: float32 [131072], P(('batch', 'g'))
- payload: bfloat16 [131072, 896], P(('batch', 'g'))
Outputs:
- output 1: float32 [262144], P(('batch', 'g'))
- output 2: bfloat16 [262144, 896], P(('batch', 'g'))
- output 3: int32 [128], P(('batch', 'g'))
All inputs are finite; a program needn't handle non-finite values.
Results may differ from the reference program's by a relative error of at most 0.001.
Values are sent between devices in bfloat16 or wider.
A program may use at most 1 GiB of HBM per device.

```python
import math
import functools
import jax
import jax.numpy as jnp
from jax import lax

GROUP = 128
N_DEV = 1024
WIDTH = 896
SEGMENTS = 16
PART_ROWS = GROUP * N_DEV
OUT_ROWS = 2 * N_DEV
PAD_KEY = 128.0


def swap_into(perm_row, dev_id, target):
    cur_pos = jnp.argmax(perm_row == dev_id)
    displaced = perm_row[target]
    slot_ids = jnp.arange(perm_row.shape[0])
    return jnp.where(slot_ids == target, dev_id, jnp.where(slot_ids == cur_pos, displaced, perm_row))


def draw_keys(base):
    k_gap, k_exp, k_pick, k_block, k_heads, k_rest, k_local = jax.random.split(base, 7)
    seg_exp = jax.random.randint(k_exp, (SEGMENTS, 1), 0, 8)
    raw_bits = jax.random.randint(k_gap, (SEGMENTS, PART_ROWS // SEGMENTS), 0, 128)
    levels = jnp.cumsum((1 + jnp.right_shift(raw_bits, 7 - seg_exp)).reshape(-1))
    centered = levels - levels[PART_ROWS // 2]
    key_scale = 2.0 ** -(int(math.log2(PART_ROWS)) + 2)
    ranked_keys = centered.astype(jnp.float32) * key_scale
    picked = jax.random.permutation(k_pick, GROUP)
    hot_dev = picked[0]
    cold_dev = picked[1]
    hot_block = jax.random.randint(k_block, (), 0, GROUP - 1)
    block_ids = jnp.arange(GROUP)[:, None]
    head_owner = jax.vmap(functools.partial(jax.random.permutation, x=GROUP))(jax.random.split(k_heads, GROUP))
    hot_row = head_owner[hot_block]
    hot_pos = jnp.argmax(hot_row == hot_dev)
    hot_row = swap_into(hot_row, hot_dev, jnp.where(hot_pos >= GROUP // 2, hot_pos, GROUP - 1))
    head_owner = jnp.where(block_ids == hot_block, hot_row[None, :], head_owner)
    next_row = swap_into(head_owner[hot_block + 1], hot_dev, 0)
    head_owner = jnp.where(block_ids == hot_block + 1, next_row[None, :], head_owner)
    tail_owner = jnp.broadcast_to(jnp.repeat(jnp.arange(GROUP), N_DEV // GROUP - 1)[None, :], (GROUP, N_DEV - GROUP))
    tail_owner = jnp.where((block_ids == hot_block) & (tail_owner == cold_dev), hot_dev, tail_owner)
    tail_owner = jnp.where((block_ids == hot_block + 1) & (tail_owner == hot_dev), cold_dev, tail_owner)
    tail_owner = jax.vmap(jax.random.permutation)(jax.random.split(k_rest, GROUP), tail_owner)
    owners = jnp.concatenate([head_owner, tail_owner], axis=1).reshape(-1)
    rank_grid = jnp.argsort(owners, stable=True).reshape(GROUP, N_DEV)
    rank_grid = jax.vmap(jax.random.permutation)(jax.random.split(k_local, GROUP), rank_grid)
    return ranked_keys[rank_grid.reshape(-1)]


def setup_inputs(seed: int = 0, part: int = 0) -> dict:
    base = jax.random.fold_in(jax.random.key(seed), part)
    k_keys, k_rows = jax.random.split(base)
    keys = draw_keys(k_keys)
    payload = jax.random.normal(k_rows, (PART_ROWS, WIDTH), jnp.float32).astype(jnp.bfloat16)
    return {"keys": keys, "payload": payload}


def reference(keys, payload):
    local_sorted = jnp.sort(keys.reshape(GROUP, N_DEV), axis=1)
    samples = local_sorted[:, :: N_DEV // GROUP].reshape(-1)
    splitters = jnp.sort(samples)[GROUP + GROUP // 2 :: GROUP]
    sorted_all, sort_order = lax.sort((keys, jnp.arange(PART_ROWS, dtype=jnp.int32)), num_keys=1)
    edges = jnp.searchsorted(sorted_all, splitters, side="left").astype(jnp.int32)
    starts = jnp.concatenate([jnp.zeros((1,), jnp.int32), edges])
    stops = jnp.concatenate([edges, jnp.full((1,), PART_ROWS, jnp.int32)])
    counts = stops - starts
    slot_ids = jnp.arange(OUT_ROWS, dtype=jnp.int32)
    src_pos = jnp.minimum(starts[:, None] + slot_ids[None, :], PART_ROWS - 1)
    is_valid = slot_ids[None, :] < counts[:, None]
    out_keys = jnp.where(is_valid, sorted_all[src_pos], PAD_KEY)
    out_payload = jnp.where(is_valid[:, :, None], payload[sort_order[src_pos]], 0.0)
    return out_keys.reshape(-1), out_payload.reshape(-1, WIDTH), counts
```

```python
import functools
import jax
import jax.numpy as jnp
from jax import lax
from jax.sharding import PartitionSpec as P
from jax.experimental import pallas as pl
from jax.experimental.pallas import tpu as pltpu

PAD_KEY = 128.0
G = 128
N = 1024
W = 896
T = 7
CAP = 16
OUT = 2048
MESH = pl.DeviceIdType.MESH


def lane_iota(shape):
    return lax.broadcasted_iota(jnp.int32, shape, 1)


def sub_iota(shape):
    return lax.broadcasted_iota(jnp.int32, shape, 0)


def exchange_kernel(
    keys_ref, pay_hbm, rk_ref, rows_hbm,
    pay_b, pay_f, stage, sendbuf, samp, runs, kbuf, rk, srt, tab_v, st_v, tab_s, st_s,
    in_sem, tab_sem, self_sem, s_send, s_recv, k_send, k_recv, p_send, p_recv,
):
    me = lax.axis_index("g")
    barrier = pltpu.get_barrier_semaphore()

    def peer(k):
        return lax.rem(me + k, G)

    def greet(k, c):
        pl.semaphore_signal(barrier, inc=1, device_id={"g": peer(k)}, device_id_type=MESH)
        return c

    load = pltpu.make_async_copy(pay_hbm, pay_b, in_sem)
    load.start()
    lax.fori_loop(1, G, greet, 0)

    keys = keys_ref[...]
    keys_t = jnp.transpose(keys)
    rank_cols = []
    for a in range(8):
        col = keys_t[:, a : a + 1]
        acc = jnp.zeros((G, 128), jnp.int32)
        for b in range(8):
            acc = acc + (keys[b : b + 1, :] < col).astype(jnp.int32)
        rank_cols.append(jnp.sum(acc, axis=1, keepdims=True))
    samples = jnp.zeros((1, 128), jnp.float32)
    for a in range(8):
        hit = rank_cols[a] == lane_iota((G, 128)) * 8
        samples = samples + jnp.sum(jnp.where(hit, keys_t[:, a : a + 1], 0.0), axis=0, keepdims=True)
    samp[...] = samples
    for r in range(8):
        want = lane_iota((G, 128)) + r * 128
        ks = jnp.zeros((G, 128), jnp.float32)
        ps = jnp.zeros((G, 128), jnp.int32)
        for a in range(8):
            hit = rank_cols[a] == want
            src = sub_iota((G, 128)) + a * 128
            addr = (src >> 3) * (8 * T) + (src & 7)
            ks = ks + jnp.where(hit, keys_t[:, a : a + 1], 0.0)
            ps = ps + jnp.where(hit, addr, 0)
        srt[r : r + 1, :] = jnp.sum(ks, axis=0, keepdims=True)
        tab_v[r : r + 1, :] = jnp.sum(ps, axis=0, keepdims=True)
    tab_v[8:16, :] = jnp.zeros((8, 128), jnp.int32)
    tab_copy = pltpu.make_async_copy(tab_v, tab_s, tab_sem)
    tab_copy.start()

    pl.semaphore_wait(barrier, G - 1)

    def send_samples(k, c):
        pltpu.make_async_remote_copy(
            src_ref=samp, dst_ref=runs.at[pl.ds(me, 1), :], send_sem=s_send, recv_sem=s_recv,
            device_id={"g": peer(k)}, device_id_type=MESH,
        ).start()
        return c

    lax.fori_loop(1, G, send_samples, 0)

    load.wait()

    def widen(g, c):
        x = pay_b[pl.ds(pl.multiple_of(g * 16, 16), 16), :].astype(jnp.float32)
        base = pl.multiple_of(g * (16 * T), 16)
        for h in range(2):
            for t in range(T):
                pay_f[pl.ds(base + h * 8 * T + t * 8, 8), :] = x[h * 8 : h * 8 + 8, t * 128 : t * 128 + 128]
        return c

    lax.fori_loop(0, N // 16, widen, 0)
    tab_copy.wait()

    pltpu.make_async_copy(runs.at[pl.ds(0, G - 1), :], runs.at[pl.ds(0, G - 1), :], s_recv).wait()
    pltpu.make_async_copy(runs.at[pl.ds(0, G - 1), :], runs.at[pl.ds(0, G - 1), :], s_send).wait()
    runs[pl.ds(me, 1), :] = samp[...]

    queries = [jnp.broadcast_to(srt[b : b + 1, :], (8, 128)) for b in range(8)]

    def count(sg, accs):
        run = runs[pl.ds(pl.multiple_of(sg * 8, 8), 8), :]
        out = []
        for b in range(8):
            pos = jnp.zeros((8, 128), jnp.int32)
            for step in (64, 32, 16, 8, 4, 2, 1, 1):
                v = jnp.take_along_axis(run, pos + (step - 1), axis=1)
                pos = pos + jnp.where(v <= queries[b], step, 0)
            out.append(accs[b] + pos)
        return tuple(out)

    accs = lax.fori_loop(0, 16, count, tuple(jnp.zeros((8, 128), jnp.int32) for _ in range(8)))
    reach = jnp.concatenate([jnp.sum(a, axis=0, keepdims=True) for a in accs], axis=0)
    reach_t = jnp.transpose(reach)
    lanes = lane_iota((G, 128))
    lo = jnp.where(lanes == 0, 0, lanes * 128 + 65)
    hi = jnp.where(lanes == 127, 1 << 20, lanes * 128 + (128 + 65))
    start = jnp.zeros((G, 128), jnp.int32)
    stop = jnp.zeros((G, 128), jnp.int32)
    for b in range(8):
        col = reach_t[:, b : b + 1]
        start = start + (col < lo).astype(jnp.int32)
        stop = stop + (col < hi).astype(jnp.int32)
    start = jnp.sum(start, axis=0, keepdims=True)
    stop = jnp.sum(stop, axis=0, keepdims=True)
    st_v[...] = start
    st_copy = pltpu.make_async_copy(st_v, st_s, tab_sem)
    st_copy.start()

    pair_t = jnp.transpose(jnp.concatenate([start, stop, jnp.zeros((6, 128), jnp.int32)], axis=0))
    tables = [jnp.broadcast_to(srt[b : b + 1, :], (8, 128)) for b in range(8)]
    for dg in range(16):
        first = pair_t[dg * 8 : dg * 8 + 8, 0:1]
        last = pair_t[dg * 8 : dg * 8 + 8, 1:2]
        slot = lane_iota((8, 128))
        idx = first + slot
        pick = idx & 127
        part = idx >> 7
        val = jnp.full((8, 128), PAD_KEY, jnp.float32)
        for b in range(8):
            val = jnp.where(part == b, jnp.take_along_axis(tables[b], pick, axis=1), val)
        kbuf[dg * 8 : dg * 8 + 8, :] = jnp.where((idx < last) & (slot < CAP), val, PAD_KEY)

    def send_keys(k, c):
        p = peer(k)
        pltpu.make_async_remote_copy(
            src_ref=kbuf.at[pl.ds(p, 1), :], dst_ref=rk.at[pl.ds(me, 1), :], send_sem=k_send, recv_sem=k_recv,
            device_id={"g": p}, device_id_type=MESH,
        ).start()
        return c

    lax.fori_loop(1, G, send_keys, 0)
    st_copy.wait()

    def build(d):
        first = st_s[0, d]
        for t in range(CAP):
            pos = first + t
            addr = tab_s[pos >> 7, pos & 127]
            stage[pl.ds((t // 8) * 8 * T + (t % 8), T, stride=8), :] = pay_f[pl.ds(addr, T, stride=8), :]
        for c in range(T):
            block = jnp.concatenate(
                [stage[c * 8 : c * 8 + 8, :], stage[8 * T + c * 8 : 8 * T + c * 8 + 8, :]], axis=0)
            sendbuf[d, :, c * 128 : c * 128 + 128] = block.astype(jnp.bfloat16)

    def send_rows(k, c):
        p = peer(k)
        build(p)
        pltpu.make_async_remote_copy(
            src_ref=sendbuf.at[p], dst_ref=rows_hbm.at[me], send_sem=p_send, recv_sem=p_recv,
            device_id={"g": p}, device_id_type=MESH,
        ).start()
        return c

    lax.fori_loop(1, G, send_rows, 0)
    build(me)
    own = pltpu.make_async_copy(sendbuf.at[me], rows_hbm.at[me], self_sem)
    own.start()
    own.wait()

    pltpu.make_async_copy(rk.at[pl.ds(0, G - 1), :], rk.at[pl.ds(0, G - 1), :], k_recv).wait()
    pltpu.make_async_copy(rk.at[pl.ds(0, G - 1), :], rk.at[pl.ds(0, G - 1), :], k_send).wait()
    rk[pl.ds(me, 1), :] = kbuf[pl.ds(me, 1), :]
    rk_ref[...] = rk[...]
    pltpu.make_async_copy(rows_hbm.at[pl.ds(0, G - 1)], rows_hbm.at[pl.ds(0, G - 1)], p_recv).wait()
    pltpu.make_async_copy(rows_hbm.at[pl.ds(0, G - 1)], rows_hbm.at[pl.ds(0, G - 1)], p_send).wait()


def exchange(keys8, rows):
    return pl.pallas_call(
        exchange_kernel,
        out_shape=(
            jax.ShapeDtypeStruct((G, 128), jnp.float32),
            jax.ShapeDtypeStruct((G, CAP, W), jnp.bfloat16),
        ),
        in_specs=[pl.BlockSpec(memory_space=pltpu.VMEM), pl.BlockSpec(memory_space=pl.ANY)],
        out_specs=(pl.BlockSpec(memory_space=pltpu.VMEM), pl.BlockSpec(memory_space=pl.ANY)),
        scratch_shapes=[
            pltpu.VMEM((N, W), jnp.bfloat16),
            pltpu.VMEM((N * T, 128), jnp.float32),
            pltpu.VMEM((16 * T, 128), jnp.float32),
            pltpu.VMEM((G, CAP, W), jnp.bfloat16),
            pltpu.VMEM((1, 128), jnp.float32),
            pltpu.VMEM((G, 128), jnp.float32),
            pltpu.VMEM((G, 128), jnp.float32),
            pltpu.VMEM((G, 128), jnp.float32),
            pltpu.VMEM((8, 128), jnp.float32),
            pltpu.VMEM((16, 128), jnp.int32),
            pltpu.VMEM((1, 128), jnp.int32),
            pltpu.SMEM((16, 128), jnp.int32),
            pltpu.SMEM((1, 128), jnp.int32),
        ] + [pltpu.SemaphoreType.DMA(())] * 9,
        compiler_params=pltpu.CompilerParams(
            collective_id=1, has_side_effects=True, vmem_limit_bytes=48 << 20),
    )(keys8, rows)


def order_kernel(rk_ref, rows_hbm, keys_out, pay_hbm, cnt_ref,
                 rows_b, rows_f, stage, outb, tab_v, tab_s, in_sem, tab_sem, out_sem):
    CH = 8
    per = OUT // CH
    loads = [
        pltpu.make_async_copy(rows_hbm.at[pl.ds(i * per, per), :], rows_b.at[pl.ds(i * per, per), :], in_sem.at[i])
        for i in range(CH)
    ]
    for l in loads:
        l.start()
    rk = rk_ref[...]
    kt = jnp.transpose(rk)[0:CAP, :]
    valid = (kt < PAD_KEY).astype(jnp.int32)
    n_valid = jnp.sum(jnp.sum(valid, axis=1, keepdims=True), axis=0, keepdims=True)
    cnt_ref[...] = jnp.broadcast_to(n_valid, (1, 128))
    rank_cols = []
    for t in range(CAP):
        col = rk[:, t : t + 1]
        acc = jnp.zeros((G, 128), jnp.int32)
        for u in range(CAP):
            acc = acc + (kt[u : u + 1, :] < col).astype(jnp.int32)
        rank_cols.append(jnp.sum(acc, axis=1, keepdims=True))
    for r in range(OUT // 128):
        want = lane_iota((G, 128)) + r * 128
        ks = jnp.zeros((G, 128), jnp.float32)
        ps = jnp.zeros((G, 128), jnp.int32)
        for t in range(CAP):
            hit = rank_cols[t] == want
            src = sub_iota((G, 128)) * CAP + t
            addr = (src >> 3) * (8 * T) + (src & 7)
            ks = ks + jnp.where(hit, rk[:, t : t + 1], 0.0)
            ps = ps + jnp.where(hit, addr, 0)
        live = (lane_iota((1, 128)) + r * 128) < n_valid
        keys_out[r : r + 1, :] = jnp.where(live, jnp.sum(ks, axis=0, keepdims=True), PAD_KEY)
        tab_v[r : r + 1, :] = jnp.where(live, jnp.sum(ps, axis=0, keepdims=True), OUT * T)
    tab = pltpu.make_async_copy(tab_v, tab_s, tab_sem)
    tab.start()
    rows_f[pl.ds(OUT * T, 8 * T), :] = jnp.zeros((8 * T, 128), jnp.float32)

    def widen(g, c):
        x = rows_b[pl.ds(pl.multiple_of(g * 16, 16), 16), :].astype(jnp.float32)
        base = pl.multiple_of(g * (16 * T), 16)
        for h in range(2):
            for t in range(T):
                rows_f[pl.ds(base + h * 8 * T + t * 8, 8), :] = x[h * 8 : h * 8 + 8, t * 128 : t * 128 + 128]
        return c

    for i in range(CH):
        loads[i].wait()
        lax.fori_loop(i * per // 16, (i + 1) * per // 16, widen, 0)
    tab.wait()

    def place(g, c):
        for t in range(16):
            pos = g * 16 + t
            addr = tab_s[pos >> 7, pos & 127]
            stage[pl.ds((t // 8) * 8 * T + (t % 8), T, stride=8), :] = rows_f[pl.ds(addr, T, stride=8), :]
        for q in range(T):
            block = jnp.concatenate(
                [stage[q * 8 : q * 8 + 8, :], stage[8 * T + q * 8 : 8 * T + q * 8 + 8, :]], axis=0)
            outb[pl.ds(pl.multiple_of(g * 16, 16), 16), q * 128 : q * 128 + 128] = block.astype(jnp.bfloat16)
        return c

    outs = []
    for i in range(CH):
        lax.fori_loop(i * per // 16, (i + 1) * per // 16, place, 0)
        o = pltpu.make_async_copy(outb.at[pl.ds(i * per, per), :], pay_hbm.at[pl.ds(i * per, per), :], out_sem.at[i])
        o.start()
        outs.append(o)
    for o in outs:
        o.wait()


def reorder(rk, rows):
    return pl.pallas_call(
        order_kernel,
        out_shape=(
            jax.ShapeDtypeStruct((OUT // 128, 128), jnp.float32),
            jax.ShapeDtypeStruct((OUT, W), jnp.bfloat16),
            jax.ShapeDtypeStruct((1, 128), jnp.int32),
        ),
        in_specs=[pl.BlockSpec(memory_space=pltpu.VMEM), pl.BlockSpec(memory_space=pl.ANY)],
        out_specs=(pl.BlockSpec(memory_space=pltpu.VMEM), pl.BlockSpec(memory_space=pl.ANY), pl.BlockSpec(memory_space=pltpu.VMEM)),
        scratch_shapes=[
            pltpu.VMEM((OUT, W), jnp.bfloat16),
            pltpu.VMEM((OUT * T + 8 * T, 128), jnp.float32),
            pltpu.VMEM((16 * T, 128), jnp.float32),
            pltpu.VMEM((OUT, W), jnp.bfloat16),
            pltpu.VMEM((16, 128), jnp.int32),
            pltpu.SMEM((16, 128), jnp.int32),
            pltpu.SemaphoreType.DMA((8,)),
            pltpu.SemaphoreType.DMA(()),
            pltpu.SemaphoreType.DMA((8,)),
        ],
        compiler_params=pltpu.CompilerParams(vmem_limit_bytes=48 << 20),
    )(rk, rows)


def solution(mesh):
    def local_part(keys_loc, rows_loc):
        rk, recv = exchange(keys_loc.reshape(8, 128), rows_loc)
        keys_out, rows_out, cnt = reorder(rk, recv.reshape(OUT, W))
        return keys_out.reshape(-1), rows_out, cnt[0, 0:1]

    row = P(("batch", "g"))
    mat = P(("batch", "g"), None)
    return jax.shard_map(local_part, mesh=mesh, in_specs=(row, mat), out_specs=(row, mat, row), check_vma=False)
```

```python
import functools
import jax
import jax.numpy as jnp
from jax import lax
from jax.sharding import PartitionSpec as P
from jax.experimental import pallas as pl
from jax.experimental.pallas import tpu as pltpu

PAD_KEY = 128.0
G = 128
N = 1024
W = 896
T = 7
CAP = 16
OUT = 2048
STRIDE = 11
PER = 16
MESH = pl.DeviceIdType.MESH


def lane_iota(shape):
    return lax.broadcasted_iota(jnp.int32, shape, 1)


def sub_iota(shape):
    return lax.broadcasted_iota(jnp.int32, shape, 0)


def exchange_kernel(
    keys_hbm, pay_hbm, rows_f, tab_ref, keys_out, cnt_ref,
    keys_v, pay_b, pay_f, stage, sendbuf, recv, samp, runs, kbuf, rk, srt, tab_v, st_v, tab_s, st_s,
    key_sem, in_sem, tab_sem, self_sem, s_send, s_recv, k_send, k_recv, p_send, p_recv,
):
    me = lax.axis_index("g")
    barrier = pltpu.get_barrier_semaphore()

    def peer(k):
        return (me + k * STRIDE) & (G - 1)

    def greet(k, c):
        pl.semaphore_signal(barrier, inc=1, device_id={"g": peer(k)}, device_id_type=MESH)
        return c

    key_load = pltpu.make_async_copy(keys_hbm, keys_v, key_sem)
    key_load.start()
    load = pltpu.make_async_copy(pay_hbm, pay_b, in_sem)
    load.start()
    lax.fori_loop(1, G, greet, 0)
    key_load.wait()

    keys = keys_v[...]
    keys_t = jnp.transpose(keys)
    rank_cols = []
    for a in range(8):
        col = keys_t[:, a : a + 1]
        acc = jnp.zeros((G, 128), jnp.int32)
        for b in range(8):
            acc = acc + (keys[b : b + 1, :] < col).astype(jnp.int32)
        rank_cols.append(jnp.sum(acc, axis=1, keepdims=True))
    for r in range(8):
        want = lane_iota((G, 128)) * 8 + r
        ks = jnp.zeros((G, 128), jnp.float32)
        ps = jnp.zeros((G, 128), jnp.int32)
        for a in range(8):
            hit = rank_cols[a] == want
            src = sub_iota((G, 128)) + a * 128
            addr = (src >> 3) * (8 * T) + (src & 7)
            ks = ks + jnp.where(hit, keys_t[:, a : a + 1], 0.0)
            ps = ps + jnp.where(hit, addr, 0)
        row = jnp.sum(ks, axis=0, keepdims=True)
        srt[r : r + 1, :] = row
        if r == 0:
            samp[...] = row
        tab_v[r : r + 1, :] = jnp.sum(ps, axis=0, keepdims=True)
    tab_copy = pltpu.make_async_copy(tab_v, tab_s, tab_sem)
    tab_copy.start()

    pl.semaphore_wait(barrier, G - 1)

    def send_samples(k, c):
        pltpu.make_async_remote_copy(
            src_ref=samp, dst_ref=runs.at[pl.ds(me, 1), :], send_sem=s_send, recv_sem=s_recv,
            device_id={"g": peer(k)}, device_id_type=MESH,
        ).start()
        return c

    lax.fori_loop(1, G, send_samples, 0)

    load.wait()

    def widen_rows(g, c):
        x = pay_b[pl.ds(pl.multiple_of(g * 16, 16), 16), :].astype(jnp.float32)
        base = pl.multiple_of(g * (16 * T), 16)
        for h in range(2):
            for t in range(T):
                pay_f[pl.ds(base + h * 8 * T + t * 8, 8), :] = x[h * 8 : h * 8 + 8, t * 128 : t * 128 + 128]
        return c

    lax.fori_loop(0, N // 16, widen_rows, 0)
    tab_copy.wait()

    many = runs.at[pl.ds(0, G - 1), :]
    pltpu.make_async_copy(many, many, s_recv).wait()
    pltpu.make_async_copy(many, many, s_send).wait()
    runs[pl.ds(me, 1), :] = samp[...]

    def reach(q_col):
        q = jnp.broadcast_to(q_col, (G, 128))

        def step(i, acc):
            for u in range(8):
                acc = acc + (runs[pl.ds(i * 8 + u, 1), :] <= q).astype(jnp.int32)
            return acc

        return jnp.sum(lax.fori_loop(0, G // 8, step, jnp.zeros((G, 128), jnp.int32)), axis=1, keepdims=True)

    sorted8 = srt[...]
    sorted8_t = jnp.transpose(sorted8)
    lanes = lane_iota((G, 128))
    need_row = jnp.where(lanes == 0, 0, lanes * 128 + 65)
    below = (reach(sorted8_t[:, 0:1]) < need_row).astype(jnp.int32)
    n_row = jnp.sum(below, axis=0, keepdims=True)
    at = jnp.broadcast_to(jnp.maximum(n_row - 1, 0), (8, 128))
    near = jnp.take_along_axis(sorted8, at, axis=1)
    near_t = jnp.transpose(near)
    n_t = jnp.transpose(jnp.broadcast_to(n_row, (8, 128)))[:, 0:1]
    dests = lax.broadcasted_iota(jnp.int32, (G, 1), 0)
    need = jnp.where(dests == 0, 0, dests * 128 + 65)
    pos = jnp.zeros((G, 1), jnp.int32)
    for width in (4, 2, 1):
        q = jnp.zeros((G, 1), jnp.float32)
        for j in range(width, 8, 2 * width):
            q = jnp.where(pos + width == j, near_t[:, j : j + 1], q)
        pos = pos + jnp.where(reach(q) < need, width, 0)
    start_col = jnp.where(n_t > 0, (n_t - 1) * 8 + pos + 1, 0)
    start = jnp.transpose(jnp.broadcast_to(start_col, (G, 128)))[0:1, :]
    stop = jnp.where(lanes[0:1, :] == G - 1, N, pltpu.roll(start, G - 1, 1))
    st_v[...] = start
    st_copy = pltpu.make_async_copy(st_v, st_s, tab_sem)
    st_copy.start()

    stop_col = jnp.transpose(jnp.broadcast_to(stop, (8, 128)))[:, 0:1]
    tables = [jnp.broadcast_to(sorted8[b : b + 1, :], (8, 128)) for b in range(8)]
    for dg in range(16):
        first = start_col[dg * 8 : dg * 8 + 8, :]
        last = stop_col[dg * 8 : dg * 8 + 8, :]
        slot = lane_iota((8, 128))
        idx = first + slot
        pick = (idx >> 3) & 127
        part = idx & 7
        val = jnp.full((8, 128), PAD_KEY, jnp.float32)
        for b in range(8):
            val = jnp.where(part == b, jnp.take_along_axis(tables[b], pick, axis=1), val)
        kbuf[dg * 8 : dg * 8 + 8, :] = jnp.where((idx < last) & (slot < CAP), val, PAD_KEY)
    st_copy.wait()

    def build(d):
        first = st_s[0, d]
        for t in range(CAP):
            pos = jnp.minimum(first + t, N - 1)
            addr = tab_s[pos & 7, pos >> 3]
            stage[pl.ds((t // 8) * 8 * T + (t % 8), T, stride=8), :] = pay_f[pl.ds(addr, T, stride=8), :]
        for c in range(T):
            block = jnp.concatenate(
                [stage[c * 8 : c * 8 + 8, :], stage[8 * T + c * 8 : 8 * T + c * 8 + 8, :]], axis=0)
            sendbuf[d, :, c * 128 : c * 128 + 128] = block.astype(jnp.bfloat16)

    def send_block(k):
        p = peer(k)
        build(p)
        pltpu.make_async_remote_copy(
            src_ref=sendbuf.at[p], dst_ref=recv.at[me], send_sem=p_send, recv_sem=p_recv.at[k // PER],
            device_id={"g": p}, device_id_type=MESH,
        ).start()

    def send_keys(k):
        p = peer(k)
        pltpu.make_async_remote_copy(
            src_ref=kbuf.at[pl.ds(p, 1), :], dst_ref=rk.at[pl.ds(me, 1), :], send_sem=k_send, recv_sem=k_recv,
            device_id={"g": p}, device_id_type=MESH,
        ).start()

    def send_both(i, c):
        send_block(i + 1)
        for u in range(8):
            k = i * 8 + u + 1

            @pl.when(k < G)
            def _():
                send_keys(k)
        return c

    lax.fori_loop(0, G // 8, send_both, 0)

    def send_rows(k, c):
        send_block(k)
        return c

    lax.fori_loop(G // 8 + 1, G, send_rows, 0)
    build(me)
    own = pltpu.make_async_copy(sendbuf.at[me], recv.at[me], self_sem)
    own.start()

    many_k = rk.at[pl.ds(0, G - 1), :]
    pltpu.make_async_copy(many_k, many_k, k_recv).wait()
    pltpu.make_async_copy(many_k, many_k, k_send).wait()
    rk[pl.ds(me, 1), :] = kbuf[pl.ds(me, 1), :]
    got = rk[...]
    kt = jnp.transpose(got)[0:CAP, :]
    valid = (kt < PAD_KEY).astype(jnp.int32)
    n_valid = jnp.sum(jnp.sum(valid, axis=1, keepdims=True), axis=0, keepdims=True)
    cnt_ref[...] = jnp.broadcast_to(n_valid, (1, 128))
    cols = []
    for t in range(CAP):
        col = got[:, t : t + 1]
        acc = jnp.zeros((G, 128), jnp.int32)
        for u in range(CAP):
            acc = acc + (kt[u : u + 1, :] < col).astype(jnp.int32)
        cols.append(jnp.sum(acc, axis=1, keepdims=True))
    places = []
    for r in range(OUT // 128):
        want = lane_iota((G, 128)) + r * 128
        wish = lane_iota((G, 128)) * 16 + r
        ks = jnp.zeros((G, 128), jnp.float32)
        ps = jnp.zeros((G, 128), jnp.int32)
        for t in range(CAP):
            src = sub_iota((G, 128)) * CAP + t
            addr = (src >> 3) * (8 * T) + (src & 7)
            ks = ks + jnp.where(cols[t] == want, got[:, t : t + 1], 0.0)
            ps = ps + jnp.where(cols[t] == wish, addr, 0)
        live = want[0:1, :] < n_valid
        keys_out[r : r + 1, :] = jnp.where(live, jnp.sum(ks, axis=0, keepdims=True), PAD_KEY)
        places.append(jnp.where(wish[0:1, :] < n_valid, jnp.sum(ps, axis=0, keepdims=True), OUT * T))
    tab_ref[...] = jnp.transpose(jnp.concatenate(places, axis=0))
    rows_f[pl.ds(OUT * T, 8 * T), :] = jnp.zeros((8 * T, 128), jnp.float32)

    def widen_block(src):
        x = recv[src].astype(jnp.float32)
        base = pl.multiple_of(src * (16 * T), 16)
        for h in range(2):
            for t in range(T):
                rows_f[pl.ds(base + h * 8 * T + t * 8, 8), :] = x[h * 8 : h * 8 + 8, t * 128 : t * 128 + 128]

    own.wait()
    widen_block(me)
    for g in range(G // PER):
        n = PER - 1 if g == 0 else PER
        part = recv.at[pl.ds(0, n)]
        pltpu.make_async_copy(part, part, p_recv.at[g]).wait()

        def widen_from(k, c):
            widen_block((me - k * STRIDE) & (G - 1))
            return c

        lax.fori_loop(max(1, g * PER), (g + 1) * PER, widen_from, 0)
    sent = sendbuf.at[pl.ds(0, G - 1)]
    pltpu.make_async_copy(sent, sent, p_send).wait()


def exchange(keys8, rows):
    vmem = pl.BlockSpec(memory_space=pltpu.VMEM)
    hbm = pl.BlockSpec(memory_space=pltpu.HBM)
    return pl.pallas_call(
        exchange_kernel,
        out_shape=(
            jax.ShapeDtypeStruct(((OUT + 8) * T, 128), jnp.float32),
            jax.ShapeDtypeStruct((G, 16), jnp.int32),
            jax.ShapeDtypeStruct((OUT // 128, 128), jnp.float32),
            jax.ShapeDtypeStruct((1, 128), jnp.int32),
        ),
        in_specs=[hbm, hbm],
        out_specs=(vmem, vmem, vmem, vmem),
        scratch_shapes=[
            pltpu.VMEM((8, 128), jnp.float32),
            pltpu.VMEM((N, W), jnp.bfloat16),
            pltpu.VMEM((N * T, 128), jnp.float32),
            pltpu.VMEM((16 * T, 128), jnp.float32),
            pltpu.VMEM((G, CAP, W), jnp.bfloat16),
            pltpu.VMEM((G, CAP, W), jnp.bfloat16),
            pltpu.VMEM((1, 128), jnp.float32),
            pltpu.VMEM((G, 128), jnp.float32),
            pltpu.VMEM((G, 128), jnp.float32),
            pltpu.VMEM((G, 128), jnp.float32),
            pltpu.VMEM((8, 128), jnp.float32),
            pltpu.VMEM((8, 128), jnp.int32),
            pltpu.VMEM((1, 128), jnp.int32),
            pltpu.SMEM((8, 128), jnp.int32),
            pltpu.SMEM((1, 128), jnp.int32),
        ] + [pltpu.SemaphoreType.DMA(())] * 9 + [pltpu.SemaphoreType.DMA((G // PER,))],
        compiler_params=pltpu.CompilerParams(
            collective_id=1, has_side_effects=True, vmem_limit_bytes=40 << 20),
    )(keys8, rows)


def order_kernel(tab_s, cnt_s, rows_f, pay_hbm, stage, outb, zeros, out_sem):
    count = cnt_s[0, 0]
    rows = 128
    chunks = OUT // rows
    zeros[...] = jnp.zeros((rows, W), jnp.bfloat16)

    def store(i, src):
        return pltpu.make_async_copy(
            src, pay_hbm.at[pl.ds(pl.multiple_of(i * rows, rows), rows), :], out_sem.at[i])

    def place(g, c):
        for t in range(16):
            addr = tab_s[g, t]
            stage[pl.ds((t // 8) * 8 * T + (t % 8), T, stride=8), :] = rows_f[pl.ds(addr, T, stride=8), :]
        for q in range(T):
            block = jnp.concatenate(
                [stage[q * 8 : q * 8 + 8, :], stage[8 * T + q * 8 : 8 * T + q * 8 + 8, :]], axis=0)
            outb[pl.ds(pl.multiple_of(g * 16, 16), 16), q * 128 : q * 128 + 128] = block.astype(jnp.bfloat16)
        return c

    def empty(i, c):
        @pl.when(i * rows >= count)
        def _():
            store(i, zeros).start()
        return c

    def full(i, c):
        @pl.when(i * rows < count)
        def _():
            lax.fori_loop(i * (rows // 16), (i + 1) * (rows // 16), place, 0)
            store(i, outb.at[pl.ds(pl.multiple_of(i * rows, rows), rows), :]).start()
        return c

    def finish(i, c):
        store(i, zeros).wait()
        return c

    lax.fori_loop(0, chunks, empty, 0)
    lax.fori_loop(0, chunks, full, 0)
    lax.fori_loop(0, chunks, finish, 0)


def reorder(tab, cnt, rows_f):
    smem = pl.BlockSpec(memory_space=pltpu.SMEM)
    return pl.pallas_call(
        order_kernel,
        out_shape=jax.ShapeDtypeStruct((OUT, W), jnp.bfloat16),
        in_specs=[smem, smem, pl.BlockSpec(memory_space=pltpu.VMEM)],
        out_specs=pl.BlockSpec(memory_space=pltpu.HBM),
        scratch_shapes=[
            pltpu.VMEM((16 * T, 128), jnp.float32),
            pltpu.VMEM((OUT, W), jnp.bfloat16),
            pltpu.VMEM((128, W), jnp.bfloat16),
            pltpu.SemaphoreType.DMA((OUT // 128,)),
        ],
        compiler_params=pltpu.CompilerParams(vmem_limit_bytes=24 << 20),
    )(tab, cnt, rows_f)


def solution(mesh):
    def local_part(keys_loc, rows_loc):
        rows_f, tab, keys_out, cnt = exchange(pltpu.with_memory_space_constraint(keys_loc.reshape(8, 128), pltpu.HBM), pltpu.with_memory_space_constraint(rows_loc, pltpu.HBM))
        rows_out = reorder(tab, cnt, rows_f)
        return keys_out.reshape(-1), rows_out, cnt[0, 0:1]

    row = P(("batch", "g"))
    mat = P(("batch", "g"), None)
    return jax.shard_map(local_part, mesh=mesh, in_specs=(row, mat), out_specs=(row, mat, row), check_vma=False)
```

```python
import functools
import jax
import jax.numpy as jnp
from jax import lax
from jax.sharding import PartitionSpec as P
from jax.experimental import pallas as pl
from jax.experimental.pallas import tpu as pltpu

PAD_KEY = 128.0
G = 128
N = 1024
W = 896
T = 7
CAP = 16
OUT = 2048
STRIDE = 11
CHIPS = G // 2
HOP = 13
PART = 8
PER = 8
MESH = pl.DeviceIdType.MESH


def lane_iota(shape):
    return lax.broadcasted_iota(jnp.int32, shape, 1)


def sub_iota(shape):
    return lax.broadcasted_iota(jnp.int32, shape, 0)


def exchange_kernel(
    keys_hbm, pay_hbm, rows_f, tab_ref, keys_out, cnt_ref,
    keys_v, pay_b, pay_f, stage, sendbuf, recv, extra, samp, runs, kbuf, rk, srt, tab_v, st_v, tab_s, st_s,
    key_sem, in_sem, tab_sem, self_sem, s_send, s_recv, k_send, k_recv, p_send, f_send, p_recv, e_recv, f_recv,
):
    me = lax.axis_index("g")
    barrier = pltpu.get_barrier_semaphore()

    def peer(k):
        return (me + k * STRIDE) & (G - 1)

    core = me & 1
    chip = me // 2
    mate = me + 1 - 2 * core

    def ahead(k):
        return (chip + k * HOP) & (CHIPS - 1)

    def behind(k):
        return (chip - k * HOP) & (CHIPS - 1)

    def greet(k, c):
        pl.semaphore_signal(barrier, inc=1, device_id={"g": peer(k)}, device_id_type=MESH)
        return c

    key_load = pltpu.make_async_copy(keys_hbm, keys_v, key_sem)
    key_load.start()
    load = pltpu.make_async_copy(pay_hbm, pay_b, in_sem)
    load.start()
    lax.fori_loop(1, G, greet, 0)
    key_load.wait()

    keys = keys_v[...]
    keys_t = jnp.transpose(keys)
    rank_cols = []
    for a in range(8):
        col = keys_t[:, a : a + 1]
        acc = jnp.zeros((G, 128), jnp.int32)
        for b in range(8):
            acc = acc + (keys[b : b + 1, :] < col).astype(jnp.int32)
        rank_cols.append(jnp.sum(acc, axis=1, keepdims=True))
    for r in range(8):
        want = lane_iota((G, 128)) * 8 + r
        ks = jnp.zeros((G, 128), jnp.float32)
        ps = jnp.zeros((G, 128), jnp.int32)
        for a in range(8):
            hit = rank_cols[a] == want
            src = sub_iota((G, 128)) + a * 128
            addr = (src >> 3) * (8 * T) + (src & 7)
            ks = ks + jnp.where(hit, keys_t[:, a : a + 1], 0.0)
            ps = ps + jnp.where(hit, addr, 0)
        row = jnp.sum(ks, axis=0, keepdims=True)
        srt[r : r + 1, :] = row
        if r == 0:
            samp[...] = row
        tab_v[r : r + 1, :] = jnp.sum(ps, axis=0, keepdims=True)
    tab_copy = pltpu.make_async_copy(tab_v, tab_s, tab_sem)
    tab_copy.start()

    pl.semaphore_wait(barrier, G - 1)

    def send_samples(k, c):
        pltpu.make_async_remote_copy(
            src_ref=samp, dst_ref=runs.at[pl.ds(me, 1), :], send_sem=s_send, recv_sem=s_recv,
            device_id={"g": peer(k)}, device_id_type=MESH,
        ).start()
        return c

    lax.fori_loop(1, G, send_samples, 0)

    load.wait()

    def widen_rows(g, c):
        x = pay_b[pl.ds(pl.multiple_of(g * 16, 16), 16), :].astype(jnp.float32)
        base = pl.multiple_of(g * (16 * T), 16)
        for h in range(2):
            for t in range(T):
                pay_f[pl.ds(base + h * 8 * T + t * 8, 8), :] = x[h * 8 : h * 8 + 8, t * 128 : t * 128 + 128]
        return c

    lax.fori_loop(0, N // 16, widen_rows, 0)
    tab_copy.wait()

    many = runs.at[pl.ds(0, G - 1), :]
    pltpu.make_async_copy(many, many, s_recv).wait()
    pltpu.make_async_copy(many, many, s_send).wait()
    runs[pl.ds(me, 1), :] = samp[...]

    def reach(q_col):
        q = jnp.broadcast_to(q_col, (G, 128))

        def step(i, acc):
            for u in range(8):
                acc = acc + (runs[pl.ds(i * 8 + u, 1), :] <= q).astype(jnp.int32)
            return acc

        return jnp.sum(lax.fori_loop(0, G // 8, step, jnp.zeros((G, 128), jnp.int32)), axis=1, keepdims=True)

    sorted8 = srt[...]
    sorted8_t = jnp.transpose(sorted8)
    lanes = lane_iota((G, 128))
    need_row = jnp.where(lanes == 0, 0, lanes * 128 + 65)
    below = (reach(sorted8_t[:, 0:1]) < need_row).astype(jnp.int32)
    n_row = jnp.sum(below, axis=0, keepdims=True)
    at = jnp.broadcast_to(jnp.maximum(n_row - 1, 0), (8, 128))
    near = jnp.take_along_axis(sorted8, at, axis=1)
    near_t = jnp.transpose(near)
    n_t = jnp.transpose(jnp.broadcast_to(n_row, (8, 128)))[:, 0:1]
    dests = lax.broadcasted_iota(jnp.int32, (G, 1), 0)
    need = jnp.where(dests == 0, 0, dests * 128 + 65)
    pos = jnp.zeros((G, 1), jnp.int32)
    for width in (4, 2, 1):
        q = jnp.zeros((G, 1), jnp.float32)
        for j in range(width, 8, 2 * width):
            q = jnp.where(pos + width == j, near_t[:, j : j + 1], q)
        pos = pos + jnp.where(reach(q) < need, width, 0)
    start_col = jnp.where(n_t > 0, (n_t - 1) * 8 + pos + 1, 0)
    start = jnp.transpose(jnp.broadcast_to(start_col, (G, 128)))[0:1, :]
    stop = jnp.where(lanes[0:1, :] == G - 1, N, pltpu.roll(start, G - 1, 1))
    over = jnp.maximum(stop - start - PART, 0)
    odd = (lanes[0:1, :] & 1) == 1
    shift = jnp.where(odd, pltpu.roll(over, 1, 1), 0)
    full = jnp.where(odd & (over + shift > PART), 1, 0)
    full = jnp.max(full, axis=1, keepdims=True).astype(jnp.float32)
    shift_col = jnp.transpose(jnp.broadcast_to(shift, (8, 128)))[:, 0:1].astype(jnp.float32)
    st_v[...] = jnp.concatenate([start, over, jnp.zeros((6, 128), jnp.int32)], axis=0)
    st_copy = pltpu.make_async_copy(st_v, st_s, tab_sem)
    st_copy.start()

    stop_col = jnp.transpose(jnp.broadcast_to(stop, (8, 128)))[:, 0:1]
    tables = [jnp.broadcast_to(sorted8[b : b + 1, :], (8, 128)) for b in range(8)]
    for dg in range(16):
        first = start_col[dg * 8 : dg * 8 + 8, :]
        last = stop_col[dg * 8 : dg * 8 + 8, :]
        slot = lane_iota((8, 128))
        idx = first + slot
        pick = (idx >> 3) & 127
        part = idx & 7
        val = jnp.full((8, 128), PAD_KEY, jnp.float32)
        for b in range(8):
            val = jnp.where(part == b, jnp.take_along_axis(tables[b], pick, axis=1), val)
        val = jnp.where((idx < last) & (slot < CAP), val, PAD_KEY)
        val = jnp.where(slot == CAP, shift_col[dg * 8 : dg * 8 + 8, :], val)
        kbuf[dg * 8 : dg * 8 + 8, :] = jnp.where(slot == CAP + 1, full, val)
    st_copy.wait()

    def row_at(pos):
        pos = jnp.minimum(pos, N - 1)
        return pay_f[pl.ds(tab_s[pos & 7, pos >> 3], T, stride=8), :]

    def build(j):
        first = st_s[0, 2 * j]
        second = st_s[0, 2 * j + 1]
        split = st_s[1, 2 * j]
        for t in range(PART):
            stage[pl.ds(t, T, stride=8), :] = row_at(first + t)
            stage[pl.ds(8 * T + t, T, stride=8), :] = row_at(second + t)
            stage[pl.ds(16 * T + t, T, stride=8), :] = row_at(
                jnp.where(t < split, first + PART + t, second + PART + t - split))
        for h in range(3):
            for c in range(T):
                base = h * 8 * T + c * 8
                sendbuf[j * 3 + h, :, c * 128 : c * 128 + 128] = stage[base : base + 8, :].astype(jnp.bfloat16)

    def send_part(src, dst, to, sem):
        pltpu.make_async_remote_copy(
            src_ref=src, dst_ref=dst.at[me], send_sem=p_send, recv_sem=sem,
            device_id={"g": to}, device_id_type=MESH,
        ).start()

    def send_block(k):
        j = ahead(k)
        build(j)
        send_part(sendbuf.at[j * 3 + 2], extra, 2 * j + core, e_recv.at[k])
        send_part(sendbuf.at[j * 3], recv, 2 * j, p_recv.at[k // PER])
        send_part(sendbuf.at[j * 3 + 1], recv, 2 * j + 1, p_recv.at[k // PER])

    def send_keys(k):
        p = peer(k)
        pltpu.make_async_remote_copy(
            src_ref=kbuf.at[pl.ds(p, 1), :], dst_ref=rk.at[pl.ds(me, 1), :], send_sem=k_send, recv_sem=k_recv,
            device_id={"g": p}, device_id_type=MESH,
        ).start()

    def send_both(i, c):
        send_block(i + 1)
        for u in range(8):
            k = i * 8 + u + 1

            @pl.when(k < G)
            def _():
                send_keys(k)
        return c

    lax.fori_loop(0, G // 8, send_both, 0)

    def send_rows(k, c):
        send_block(k)
        return c

    lax.fori_loop(G // 8 + 1, CHIPS, send_rows, 0)
    build(chip)
    send_part(sendbuf.at[chip * 3 + 1 - core], recv, mate, p_recv.at[0])
    send_part(sendbuf.at[chip * 3 + 2], extra, mate, f_recv.at[0])
    own = pltpu.make_async_copy(sendbuf.at[chip * 3 + core], recv.at[me], self_sem)
    own.start()
    own_extra = pltpu.make_async_copy(sendbuf.at[chip * 3 + 2], extra.at[me], key_sem)
    own_extra.start()

    many_k = rk.at[pl.ds(0, G - 1), :]
    pltpu.make_async_copy(many_k, many_k, k_recv).wait()
    pltpu.make_async_copy(many_k, many_k, k_send).wait()
    rk[pl.ds(me, 1), :] = kbuf[pl.ds(me, 1), :]
    got = rk[...]
    kt = jnp.transpose(got)[0:CAP, :]
    valid = (kt < PAD_KEY).astype(jnp.int32)
    n_valid = jnp.sum(jnp.sum(valid, axis=1, keepdims=True), axis=0, keepdims=True)
    any_full = jnp.max(got[:, CAP + 1 : CAP + 2], axis=0, keepdims=True).astype(jnp.int32)
    cnt_ref[...] = jnp.where(lanes[0:1, :] == 0, n_valid, any_full)
    skip = got[:, CAP : CAP + 1].astype(jnp.int32)
    cols = []
    for t in range(CAP):
        col = got[:, t : t + 1]
        acc = jnp.zeros((G, 128), jnp.int32)
        for u in range(CAP):
            acc = acc + (kt[u : u + 1, :] < col).astype(jnp.int32)
        cols.append(jnp.sum(acc, axis=1, keepdims=True))
    places = []
    for r in range(OUT // 128):
        want = lane_iota((G, 128)) + r * 128
        wish = lane_iota((G, 128)) * 16 + r
        ks = jnp.zeros((G, 128), jnp.float32)
        ps = jnp.zeros((G, 128), jnp.int32)
        for t in range(CAP):
            if t < PART:
                addr = sub_iota((G, 1)) * (8 * T) + t
            else:
                addr = (sub_iota((G, 1)) + G) * (8 * T) + jnp.minimum(skip + (t - PART), PART - 1)
            ks = ks + jnp.where(cols[t] == want, got[:, t : t + 1], 0.0)
            ps = ps + jnp.where(cols[t] == wish, addr, 0)
        live = want[0:1, :] < n_valid
        keys_out[r : r + 1, :] = jnp.where(live, jnp.sum(ks, axis=0, keepdims=True), PAD_KEY)
        places.append(jnp.where(wish[0:1, :] < n_valid, jnp.sum(ps, axis=0, keepdims=True), OUT * T))
    tab_ref[...] = jnp.transpose(jnp.concatenate(places, axis=0))
    rows_f[pl.ds(OUT * T, 8 * T), :] = jnp.zeros((8 * T, 128), jnp.float32)

    def widen(part, src, first):
        x = part[src].astype(jnp.float32)
        base = pl.multiple_of((first + src) * (8 * T), 8)
        for t in range(T):
            rows_f[pl.ds(base + t * 8, 8), :] = x[:, t * 128 : t * 128 + 128]

    own.wait()
    own_extra.wait()
    widen(recv, me, 0)
    widen(extra, me, G)
    one = extra.at[0]

    def forward(k, c):
        pltpu.make_async_copy(one, one, e_recv.at[k]).wait()
        src = 2 * behind(k) + core
        pltpu.make_async_remote_copy(
            src_ref=extra.at[src], dst_ref=extra.at[src], send_sem=f_send, recv_sem=f_recv.at[k // PER],
            device_id={"g": mate}, device_id_type=MESH,
        ).start()
        return c

    def widen_direct(k, c):
        j = behind(k)
        widen(recv, 2 * j, 0)
        widen(recv, 2 * j + 1, 0)
        widen(extra, 2 * j + core, G)
        return c

    def widen_forwarded(k, c):
        widen(extra, 2 * behind(k) + 1 - core, G)
        return c

    for g in range(CHIPS // PER):
        lo = max(1, g * PER)
        hi = (g + 1) * PER
        lax.fori_loop(lo, hi, forward, 0)
        got_part = recv.at[pl.ds(0, 2 * PER - 1 if g == 0 else 2 * PER)]
        pltpu.make_async_copy(got_part, got_part, p_recv.at[g]).wait()
        if g == 0:
            widen(recv, mate, 0)
        lax.fori_loop(lo, hi, widen_direct, 0)
        if g > 0:
            fw = extra.at[pl.ds(0, PER)]
            pltpu.make_async_copy(fw, fw, f_recv.at[g - 1]).wait()
            lax.fori_loop((g - 1) * PER, g * PER, widen_forwarded, 0)
    fw = extra.at[pl.ds(0, PER)]
    pltpu.make_async_copy(fw, fw, f_recv.at[CHIPS // PER - 1]).wait()
    lax.fori_loop(CHIPS - PER, CHIPS, widen_forwarded, 0)
    sent = sendbuf.at[pl.ds(0, 3 * (CHIPS - 1) + 2)]
    pltpu.make_async_copy(sent, sent, p_send).wait()
    passed = extra.at[pl.ds(0, CHIPS - 1)]
    pltpu.make_async_copy(passed, passed, f_send).wait()


def exchange(keys8, rows):
    vmem = pl.BlockSpec(memory_space=pltpu.VMEM)
    hbm = pl.BlockSpec(memory_space=pltpu.HBM)
    return pl.pallas_call(
        exchange_kernel,
        out_shape=(
            jax.ShapeDtypeStruct(((OUT + 8) * T, 128), jnp.float32),
            jax.ShapeDtypeStruct((G, 16), jnp.int32),
            jax.ShapeDtypeStruct((OUT // 128, 128), jnp.float32),
            jax.ShapeDtypeStruct((1, 128), jnp.int32),
        ),
        in_specs=[hbm, hbm],
        out_specs=(vmem, vmem, vmem, vmem),
        scratch_shapes=[
            pltpu.VMEM((8, 128), jnp.float32),
            pltpu.VMEM((N, W), jnp.bfloat16),
            pltpu.VMEM((N * T, 128), jnp.float32),
            pltpu.VMEM((24 * T, 128), jnp.float32),
            pltpu.VMEM((3 * CHIPS, PART, W), jnp.bfloat16),
            pltpu.VMEM((G, PART, W), jnp.bfloat16),
            pltpu.VMEM((G, PART, W), jnp.bfloat16),
            pltpu.VMEM((1, 128), jnp.float32),
            pltpu.VMEM((G, 128), jnp.float32),
            pltpu.VMEM((G, 128), jnp.float32),
            pltpu.VMEM((G, 128), jnp.float32),
            pltpu.VMEM((8, 128), jnp.float32),
            pltpu.VMEM((8, 128), jnp.int32),
            pltpu.VMEM((8, 128), jnp.int32),
            pltpu.SMEM((8, 128), jnp.int32),
            pltpu.SMEM((8, 128), jnp.int32),
        ] + [pltpu.SemaphoreType.DMA(())] * 10 + [
            pltpu.SemaphoreType.DMA((CHIPS // PER,)),
            pltpu.SemaphoreType.DMA((CHIPS,)),
            pltpu.SemaphoreType.DMA((CHIPS // PER,)),
        ],
        compiler_params=pltpu.CompilerParams(
            collective_id=1, has_side_effects=True, vmem_limit_bytes=40 << 20),
    )(keys8, rows)


def order_kernel(tab_s, cnt_s, rows_f, pay_hbm, stage, outb, zeros, out_sem):
    count = cnt_s[0, 0]
    rows = 128
    chunks = OUT // rows
    zeros[...] = jnp.zeros((rows, W), jnp.bfloat16)

    def store(i, src):
        return pltpu.make_async_copy(
            src, pay_hbm.at[pl.ds(pl.multiple_of(i * rows, rows), rows), :], out_sem.at[i])

    def place(g, c):
        for t in range(16):
            addr = tab_s[g, t]
            stage[pl.ds((t // 8) * 8 * T + (t % 8), T, stride=8), :] = rows_f[pl.ds(addr, T, stride=8), :]
        for q in range(T):
            block = jnp.concatenate(
                [stage[q * 8 : q * 8 + 8, :], stage[8 * T + q * 8 : 8 * T + q * 8 + 8, :]], axis=0)
            outb[pl.ds(pl.multiple_of(g * 16, 16), 16), q * 128 : q * 128 + 128] = block.astype(jnp.bfloat16)
        return c

    def empty(i, c):
        @pl.when(i * rows >= count)
        def _():
            store(i, zeros).start()
        return c

    def full(i, c):
        @pl.when(i * rows < count)
        def _():
            lax.fori_loop(i * (rows // 16), (i + 1) * (rows // 16), place, 0)
            store(i, outb.at[pl.ds(pl.multiple_of(i * rows, rows), rows), :]).start()
        return c

    def finish(i, c):
        store(i, zeros).wait()
        return c

    lax.fori_loop(0, chunks, empty, 0)
    lax.fori_loop(0, chunks, full, 0)
    lax.fori_loop(0, chunks, finish, 0)


def reorder(tab, cnt, rows_f):
    smem = pl.BlockSpec(memory_space=pltpu.SMEM)
    return pl.pallas_call(
        order_kernel,
        out_shape=jax.ShapeDtypeStruct((OUT, W), jnp.bfloat16),
        in_specs=[smem, smem, pl.BlockSpec(memory_space=pltpu.VMEM)],
        out_specs=pl.BlockSpec(memory_space=pltpu.HBM),
        scratch_shapes=[
            pltpu.VMEM((16 * T, 128), jnp.float32),
            pltpu.VMEM((OUT, W), jnp.bfloat16),
            pltpu.VMEM((128, W), jnp.bfloat16),
            pltpu.SemaphoreType.DMA((OUT // 128,)),
        ],
        compiler_params=pltpu.CompilerParams(vmem_limit_bytes=24 << 20),
    )(tab, cnt, rows_f)


def plain_sort(keys_loc, rows_loc):
    sorted_keys, sort_order = lax.sort((keys_loc, lax.iota(jnp.int32, N)), num_keys=1)
    samples = sorted_keys[:: N // G]
    all_samples = jnp.sort(lax.all_gather(samples, "g", tiled=True))
    splitters = all_samples[G + G // 2 :: G]
    edges = jnp.searchsorted(sorted_keys, splitters, side="left").astype(jnp.int32)
    starts = jnp.concatenate([jnp.zeros((1,), jnp.int32), edges])
    stops = jnp.concatenate([edges, jnp.full((1,), N, jnp.int32)])
    src_pos = starts[:, None] + lax.iota(jnp.int32, CAP)[None, :]
    is_valid = src_pos < stops[:, None]
    src_pos = jnp.minimum(src_pos, N - 1)
    send_keys = jnp.where(is_valid, sorted_keys[src_pos], PAD_KEY)
    send_rows = jnp.where(is_valid[:, :, None], rows_loc[sort_order[src_pos]], 0.0)
    recv_keys = lax.all_to_all(send_keys, "g", 0, 0, tiled=True)
    recv_rows = lax.all_to_all(send_rows, "g", 0, 0, tiled=True)
    flat_keys = recv_keys.reshape(-1)
    merged_keys, merge_order = lax.sort((flat_keys, lax.iota(jnp.int32, OUT)), num_keys=1)
    return merged_keys, recv_rows.reshape(-1, W)[merge_order]


def solution(mesh):
    def local_part(keys_loc, rows_loc):
        rows_f, tab, keys_out, cnt = exchange(
            pltpu.with_memory_space_constraint(keys_loc.reshape(8, 128), pltpu.HBM),
            pltpu.with_memory_space_constraint(rows_loc, pltpu.HBM))
        rows_out = reorder(tab, cnt, rows_f)

        def redo(state):
            keys_all, rows_all = plain_sort(keys_loc, rows_loc)
            return jnp.int32(0), keys_all, rows_all

        _, keys_sorted, rows_sorted = lax.while_loop(
            lambda state: state[0] > 0, redo, (cnt[0, 1], keys_out.reshape(-1), rows_out))
        return keys_sorted, rows_sorted, cnt[0, 0:1]

    row = P(("batch", "g"))
    mat = P(("batch", "g"), None)
    return jax.shard_map(local_part, mesh=mesh, in_specs=(row, mat), out_specs=(row, mat, row), check_vma=False)
```

```python
import functools
import jax
import jax.numpy as jnp
from jax import lax
from jax.sharding import PartitionSpec as P
from jax.experimental import pallas as pl
from jax.experimental.pallas import tpu as pltpu

PAD_KEY = 128.0
G = 128
N = 1024
W = 896
T = 7
CAP = 16
OUT = 2048
STRIDE = 11
CHIPS = G // 2
HOP = 29
PART = 8
LAG = 21
PER = 8
MESH = pl.DeviceIdType.MESH


def lane_iota(shape):
    return lax.broadcasted_iota(jnp.int32, shape, 1)


def sub_iota(shape):
    return lax.broadcasted_iota(jnp.int32, shape, 0)


def exchange_kernel(
    keys_hbm, pay_hbm, rows_f, tab_ref, keys_out, cnt_ref,
    keys_v, pay_b, pay_f, stage, sendbuf, recv, extra, samp, runs, kbuf, rk, srt, tab_v, st_v, tab_s, st_s,
    key_sem, in_sem, tab_sem, self_sem, s_send, s_recv, k_send, k_recv, p_send, f_send, p_recv, e_recv, f_recv,
):
    me = lax.axis_index("g")
    barrier = pltpu.get_barrier_semaphore()

    def peer(k):
        return (me + k * STRIDE) & (G - 1)

    core = me & 1
    chip = me // 2
    mate = me + 1 - 2 * core

    def ahead(k):
        return (chip + k * HOP) & (CHIPS - 1)

    def behind(k):
        return (chip - k * HOP) & (CHIPS - 1)

    def greet(k, c):
        pl.semaphore_signal(barrier, inc=1, device_id={"g": peer(k)}, device_id_type=MESH)
        return c

    key_load = pltpu.make_async_copy(keys_hbm, keys_v, key_sem)
    key_load.start()
    load = pltpu.make_async_copy(pay_hbm, pay_b, in_sem)
    load.start()
    lax.fori_loop(1, G, greet, 0)
    key_load.wait()

    keys = keys_v[...]
    keys_t = jnp.transpose(keys)
    rank_cols = []
    for a in range(8):
        col = keys_t[:, a : a + 1]
        acc = jnp.zeros((G, 128), jnp.int32)
        for b in range(8):
            acc = acc + (keys[b : b + 1, :] < col).astype(jnp.int32)
        rank_cols.append(jnp.sum(acc, axis=1, keepdims=True))
    def sort_row(r):
        want = lane_iota((G, 128)) * 8 + r
        ks = jnp.zeros((G, 128), jnp.float32)
        ps = jnp.zeros((G, 128), jnp.int32)
        for a in range(8):
            hit = rank_cols[a] == want
            src = sub_iota((G, 1)) + a * 128
            addr = (src >> 3) * (8 * T) + (src & 7)
            ks = ks + jnp.where(hit, keys_t[:, a : a + 1], 0.0)
            ps = ps + jnp.where(hit, addr, 0)
        row = jnp.sum(ks, axis=0, keepdims=True)
        srt[r : r + 1, :] = row
        tab_v[r : r + 1, :] = jnp.sum(ps, axis=0, keepdims=True)
        return row

    samp[...] = sort_row(0)
    pl.semaphore_wait(barrier, G - 1)

    def send_samples(k, c):
        pltpu.make_async_remote_copy(
            src_ref=samp, dst_ref=runs.at[pl.ds(me, 1), :], send_sem=s_send, recv_sem=s_recv,
            device_id={"g": peer(k)}, device_id_type=MESH,
        ).start()
        return c

    lax.fori_loop(1, G, send_samples, 0)

    for r in range(1, 8):
        sort_row(r)
    tab_copy = pltpu.make_async_copy(tab_v, tab_s, tab_sem)
    tab_copy.start()
    load.wait()

    def widen_rows(g, c):
        x = pay_b[pl.ds(pl.multiple_of(g * 16, 16), 16), :].astype(jnp.float32)
        base = pl.multiple_of(g * (16 * T), 16)
        for h in range(2):
            for t in range(T):
                pay_f[pl.ds(base + h * 8 * T + t * 8, 8), :] = x[h * 8 : h * 8 + 8, t * 128 : t * 128 + 128]
        return c

    lax.fori_loop(0, N // 16, widen_rows, 0)
    tab_copy.wait()

    many = runs.at[pl.ds(0, G - 1), :]
    pltpu.make_async_copy(many, many, s_recv).wait()
    pltpu.make_async_copy(many, many, s_send).wait()
    runs[pl.ds(me, 1), :] = samp[...]

    def reach(q_col):
        q = jnp.broadcast_to(q_col, (G, 128))

        def step(i, acc):
            for u in range(8):
                acc = acc + (runs[pl.ds(i * 8 + u, 1), :] <= q).astype(jnp.int32)
            return acc

        return jnp.sum(lax.fori_loop(0, G // 8, step, jnp.zeros((G, 128), jnp.int32)), axis=1, keepdims=True)

    sorted8 = srt[...]
    sorted8_t = jnp.transpose(sorted8)
    lanes = lane_iota((G, 128))
    need_row = jnp.where(lanes == 0, 0, lanes * 128 + 65)
    below = (reach(sorted8_t[:, 0:1]) < need_row).astype(jnp.int32)
    n_row = jnp.sum(below, axis=0, keepdims=True)
    at = jnp.broadcast_to(jnp.maximum(n_row - 1, 0), (8, 128))
    near = jnp.take_along_axis(sorted8, at, axis=1)
    near_t = jnp.transpose(near)
    n_t = jnp.transpose(jnp.broadcast_to(n_row, (8, 128)))[:, 0:1]
    dests = lax.broadcasted_iota(jnp.int32, (G, 1), 0)
    need = jnp.where(dests == 0, 0, dests * 128 + 65)
    pos = jnp.zeros((G, 1), jnp.int32)
    for width in (4, 2, 1):
        q = jnp.zeros((G, 1), jnp.float32)
        for j in range(width, 8, 2 * width):
            q = jnp.where(pos + width == j, near_t[:, j : j + 1], q)
        pos = pos + jnp.where(reach(q) < need, width, 0)
    start_col = jnp.where(n_t > 0, (n_t - 1) * 8 + pos + 1, 0)
    start = jnp.transpose(jnp.broadcast_to(start_col, (G, 128)))[0:1, :]
    stop = jnp.where(lanes[0:1, :] == G - 1, N, pltpu.roll(start, G - 1, 1))
    over = jnp.maximum(stop - start - PART, 0)
    odd = (lanes[0:1, :] & 1) == 1
    shift = jnp.where(odd, pltpu.roll(over, 1, 1), 0)
    full = jnp.where(odd & (over + shift > PART), 1, 0)
    full = jnp.max(full, axis=1, keepdims=True).astype(jnp.float32)
    shift_col = jnp.transpose(jnp.broadcast_to(shift, (8, 128)))[:, 0:1].astype(jnp.float32)
    st_v[...] = jnp.concatenate([start, over, jnp.zeros((6, 128), jnp.int32)], axis=0)
    st_copy = pltpu.make_async_copy(st_v, st_s, tab_sem)
    st_copy.start()

    st_copy.wait()

    def row_at(pos):
        pos = jnp.minimum(pos, N - 1)
        return pay_f[pl.ds(tab_s[pos & 7, pos >> 3], T, stride=8), :]

    def build(j):
        first = st_s[0, 2 * j]
        second = st_s[0, 2 * j + 1]
        split = st_s[1, 2 * j]
        for t in range(PART):
            stage[pl.ds(t, T, stride=8), :] = row_at(first + t)
            stage[pl.ds(8 * T + t, T, stride=8), :] = row_at(second + t)
            stage[pl.ds(16 * T + t, T, stride=8), :] = row_at(
                jnp.where(t < split, first + PART + t, second + PART + t - split))
        for h in range(3):
            for c in range(T):
                base = h * 8 * T + c * 8
                sendbuf[j * 3 + h, :, c * 128 : c * 128 + 128] = stage[base : base + 8, :].astype(jnp.bfloat16)

    def send_part(src, dst, to, sem):
        pltpu.make_async_remote_copy(
            src_ref=src, dst_ref=dst.at[me], send_sem=p_send, recv_sem=sem,
            device_id={"g": to}, device_id_type=MESH,
        ).start()

    def send_c(k):
        j = ahead(k)
        build(j)
        send_part(sendbuf.at[j * 3 + 2], extra, 2 * j + core, e_recv.at[k])

    def send_a(k):
        j = ahead(k)
        send_part(sendbuf.at[j * 3], recv, 2 * j, p_recv.at[k // PER])

    def send_b(k):
        j = ahead(k)
        send_part(sendbuf.at[j * 3 + 1], recv, 2 * j + 1, p_recv.at[k // PER])

    def send_keys(k):
        p = peer(k)
        pltpu.make_async_remote_copy(
            src_ref=kbuf.at[pl.ds(p, 1), :], dst_ref=rk.at[pl.ds(me, 1), :], send_sem=k_send, recv_sem=k_recv,
            device_id={"g": p}, device_id_type=MESH,
        ).start()

    def key_steps(k, c):
        send_c(k)
        send_a(k - LAG)
        for u in range(8):
            i = (k - LAG) * 8 + u - 7

            @pl.when(i < G)
            def _():
                send_keys(i)
        return c

    def steps(lo, hi, what):
        def step(k, c):
            if "c" in what:
                send_c(k)
            if "a" in what:
                send_a(k - LAG)
            if "b" in what:
                send_b(k - 2 * LAG)
            return c

        lax.fori_loop(lo, hi, step, 0)

    steps(1, LAG + 1, "c")

    stop_col = jnp.transpose(jnp.broadcast_to(stop, (8, 128)))[:, 0:1]
    tables = [jnp.broadcast_to(sorted8[b : b + 1, :], (8, 128)) for b in range(8)]
    for dg in range(16):
        first = start_col[dg * 8 : dg * 8 + 8, :]
        last = stop_col[dg * 8 : dg * 8 + 8, :]
        slot = lane_iota((8, 128))
        idx = first + slot
        pick = (idx >> 3) & 127
        part = idx & 7
        val = jnp.full((8, 128), PAD_KEY, jnp.float32)
        for b in range(8):
            val = jnp.where(part == b, jnp.take_along_axis(tables[b], pick, axis=1), val)
        val = jnp.where((idx < last) & (slot < CAP), val, PAD_KEY)
        val = jnp.where(slot == CAP, shift_col[dg * 8 : dg * 8 + 8, :], val)
        kbuf[dg * 8 : dg * 8 + 8, :] = jnp.where(slot == CAP + 1, full, val)

    lax.fori_loop(LAG + 1, LAG + 1 + G // 8, key_steps, 0)
    steps(LAG + 1 + G // 8, 2 * LAG + 1, "ca")
    steps(2 * LAG + 1, CHIPS, "cab")
    steps(CHIPS, CHIPS + LAG, "ab")
    steps(CHIPS + LAG, CHIPS + 2 * LAG, "b")
    build(chip)
    send_part(sendbuf.at[chip * 3 + 1 - core], recv, mate, p_recv.at[0])
    send_part(sendbuf.at[chip * 3 + 2], extra, mate, f_recv.at[0])
    own = pltpu.make_async_copy(sendbuf.at[chip * 3 + core], recv.at[me], self_sem)
    own.start()
    own_extra = pltpu.make_async_copy(sendbuf.at[chip * 3 + 2], extra.at[me], key_sem)
    own_extra.start()

    many_k = rk.at[pl.ds(0, G - 1), :]
    pltpu.make_async_copy(many_k, many_k, k_recv).wait()
    pltpu.make_async_copy(many_k, many_k, k_send).wait()
    rk[pl.ds(me, 1), :] = kbuf[pl.ds(me, 1), :]
    got = rk[...]
    kt = jnp.transpose(got)[0:CAP, :]
    valid = (kt < PAD_KEY).astype(jnp.int32)
    n_valid = jnp.sum(jnp.sum(valid, axis=1, keepdims=True), axis=0, keepdims=True)
    any_full = jnp.max(got[:, CAP + 1 : CAP + 2], axis=0, keepdims=True).astype(jnp.int32)
    cnt_ref[...] = jnp.where(lanes[0:1, :] == 0, n_valid, any_full)
    skip = got[:, CAP : CAP + 1].astype(jnp.int32)
    cols = []
    for t in range(CAP):
        col = got[:, t : t + 1]
        acc = jnp.zeros((G, 128), jnp.int32)
        for u in range(CAP):
            acc = acc + (kt[u : u + 1, :] < col).astype(jnp.int32)
        cols.append(jnp.sum(acc, axis=1, keepdims=True))
    places = []
    for r in range(OUT // 128):
        want = lane_iota((G, 128)) + r * 128
        wish = lane_iota((G, 128)) * 16 + r
        ks = jnp.zeros((G, 128), jnp.float32)
        ps = jnp.zeros((G, 128), jnp.int32)
        for t in range(CAP):
            if t < PART:
                addr = sub_iota((G, 1)) * (8 * T) + t
            else:
                addr = (sub_iota((G, 1)) + G) * (8 * T) + jnp.minimum(skip + (t - PART), PART - 1)
            ks = ks + jnp.where(cols[t] == want, got[:, t : t + 1], 0.0)
            ps = ps + jnp.where(cols[t] == wish, addr, 0)
        live = want[0:1, :] < n_valid
        keys_out[r : r + 1, :] = jnp.where(live, jnp.sum(ks, axis=0, keepdims=True), PAD_KEY)
        places.append(jnp.where(wish[0:1, :] < n_valid, jnp.sum(ps, axis=0, keepdims=True), OUT * T))
    tab_ref[...] = jnp.transpose(jnp.concatenate(places, axis=0))
    rows_f[pl.ds(OUT * T, 8 * T), :] = jnp.zeros((8 * T, 128), jnp.float32)

    def widen(part, src, first):
        x = part[src].astype(jnp.float32)
        base = pl.multiple_of((first + src) * (8 * T), 8)
        for t in range(T):
            rows_f[pl.ds(base + t * 8, 8), :] = x[:, t * 128 : t * 128 + 128]

    own.wait()
    own_extra.wait()
    widen(recv, me, 0)
    widen(extra, me, G)
    one = extra.at[0]

    def forward(k, c):
        pltpu.make_async_copy(one, one, e_recv.at[k]).wait()
        src = 2 * behind(k) + core
        pltpu.make_async_remote_copy(
            src_ref=extra.at[src], dst_ref=extra.at[src], send_sem=f_send, recv_sem=f_recv.at[k // PER],
            device_id={"g": mate}, device_id_type=MESH,
        ).start()
        return c

    def widen_direct(k, c):
        j = behind(k)
        widen(recv, 2 * j, 0)
        widen(recv, 2 * j + 1, 0)
        widen(extra, 2 * j + core, G)
        return c

    def widen_forwarded(k, c):
        widen(extra, 2 * behind(k) + 1 - core, G)
        return c

    for g in range(CHIPS // PER):
        lo = max(1, g * PER)
        hi = (g + 1) * PER
        lax.fori_loop(lo, hi, forward, 0)
        got_part = recv.at[pl.ds(0, 2 * PER - 1 if g == 0 else 2 * PER)]
        pltpu.make_async_copy(got_part, got_part, p_recv.at[g]).wait()
        if g == 0:
            widen(recv, mate, 0)
        lax.fori_loop(lo, hi, widen_direct, 0)
        if g > 0:
            fw = extra.at[pl.ds(0, PER)]
            pltpu.make_async_copy(fw, fw, f_recv.at[g - 1]).wait()
            lax.fori_loop((g - 1) * PER, g * PER, widen_forwarded, 0)
    fw = extra.at[pl.ds(0, PER)]
    pltpu.make_async_copy(fw, fw, f_recv.at[CHIPS // PER - 1]).wait()
    lax.fori_loop(CHIPS - PER, CHIPS, widen_forwarded, 0)
    sent = sendbuf.at[pl.ds(0, 3 * (CHIPS - 1) + 2)]
    pltpu.make_async_copy(sent, sent, p_send).wait()
    passed = extra.at[pl.ds(0, CHIPS - 1)]
    pltpu.make_async_copy(passed, passed, f_send).wait()


def exchange(keys8, rows):
    vmem = pl.BlockSpec(memory_space=pltpu.VMEM)
    hbm = pl.BlockSpec(memory_space=pltpu.HBM)
    return pl.pallas_call(
        exchange_kernel,
        out_shape=(
            jax.ShapeDtypeStruct(((OUT + 8) * T, 128), jnp.float32),
            jax.ShapeDtypeStruct((G, 16), jnp.int32),
            jax.ShapeDtypeStruct((OUT // 128, 128), jnp.float32),
            jax.ShapeDtypeStruct((1, 128), jnp.int32),
        ),
        in_specs=[hbm, hbm],
        out_specs=(vmem, vmem, vmem, vmem),
        scratch_shapes=[
            pltpu.VMEM((8, 128), jnp.float32),
            pltpu.VMEM((N, W), jnp.bfloat16),
            pltpu.VMEM((N * T, 128), jnp.float32),
            pltpu.VMEM((24 * T, 128), jnp.float32),
            pltpu.VMEM((3 * CHIPS, PART, W), jnp.bfloat16),
            pltpu.VMEM((G, PART, W), jnp.bfloat16),
            pltpu.VMEM((G, PART, W), jnp.bfloat16),
            pltpu.VMEM((1, 128), jnp.float32),
            pltpu.VMEM((G, 128), jnp.float32),
            pltpu.VMEM((G, 128), jnp.float32),
            pltpu.VMEM((G, 128), jnp.float32),
            pltpu.VMEM((8, 128), jnp.float32),
            pltpu.VMEM((8, 128), jnp.int32),
            pltpu.VMEM((8, 128), jnp.int32),
            pltpu.SMEM((8, 128), jnp.int32),
            pltpu.SMEM((8, 128), jnp.int32),
        ] + [pltpu.SemaphoreType.DMA(())] * 10 + [
            pltpu.SemaphoreType.DMA((CHIPS // PER,)),
            pltpu.SemaphoreType.DMA((CHIPS,)),
            pltpu.SemaphoreType.DMA((CHIPS // PER,)),
        ],
        compiler_params=pltpu.CompilerParams(
            collective_id=1, has_side_effects=True, vmem_limit_bytes=40 << 20),
    )(keys8, rows)


def order_kernel(tab_s, cnt_s, rows_f, keys_v, pay_hbm, keys_hbm, cnt_hbm, flag_hbm, stage, outb, zeros, cnt_v, flag_v, out_sem, key_sem, cnt_sem, flag_sem):
    count = cnt_s[0, 0]
    cnt_v[0] = count
    flag_v[0] = cnt_s[0, 1]
    cnt_store = pltpu.make_async_copy(cnt_v, cnt_hbm, cnt_sem)
    cnt_store.start()
    flag_store = pltpu.make_async_copy(flag_v, flag_hbm, flag_sem)
    flag_store.start()
    keys_store = pltpu.make_async_copy(keys_v, keys_hbm, key_sem)
    keys_store.start()
    rows = 128
    chunks = OUT // rows
    zeros[...] = jnp.zeros((rows, W), jnp.bfloat16)

    def store(i, src):
        return pltpu.make_async_copy(
            src, pay_hbm.at[pl.ds(pl.multiple_of(i * rows, rows), rows), :], out_sem.at[i])

    def place(g, c):
        for t in range(16):
            addr = tab_s[g, t]
            stage[pl.ds((t // 8) * 8 * T + (t % 8), T, stride=8), :] = rows_f[pl.ds(addr, T, stride=8), :]
        for q in range(T):
            block = jnp.concatenate(
                [stage[q * 8 : q * 8 + 8, :], stage[8 * T + q * 8 : 8 * T + q * 8 + 8, :]], axis=0)
            outb[pl.ds(pl.multiple_of(g * 16, 16), 16), q * 128 : q * 128 + 128] = block.astype(jnp.bfloat16)
        return c

    def empty(i, c):
        @pl.when(i * rows >= count)
        def _():
            store(i, zeros).start()
        return c

    def full(i, c):
        @pl.when(i * rows < count)
        def _():
            lax.fori_loop(i * (rows // 16), (i + 1) * (rows // 16), place, 0)
            store(i, outb.at[pl.ds(pl.multiple_of(i * rows, rows), rows), :]).start()
        return c

    def finish(i, c):
        store(i, zeros).wait()
        return c

    lax.fori_loop(0, chunks, empty, 0)
    lax.fori_loop(0, chunks, full, 0)
    keys_store.wait()
    cnt_store.wait()
    flag_store.wait()
    lax.fori_loop(0, chunks, finish, 0)


def reorder(tab, cnt, rows_f, keys):
    smem = pl.BlockSpec(memory_space=pltpu.SMEM)
    vmem = pl.BlockSpec(memory_space=pltpu.VMEM)
    hbm = pl.BlockSpec(memory_space=pltpu.HBM)
    return pl.pallas_call(
        order_kernel,
        out_shape=(
            jax.ShapeDtypeStruct((OUT, W), jnp.bfloat16),
            jax.ShapeDtypeStruct((OUT // 128, 128), jnp.float32),
            jax.ShapeDtypeStruct((1,), jnp.int32),
            jax.ShapeDtypeStruct((1,), jnp.int32),
        ),
        in_specs=[smem, smem, vmem, vmem],
        out_specs=(hbm, hbm, hbm, hbm),
        scratch_shapes=[
            pltpu.VMEM((16 * T, 128), jnp.float32),
            pltpu.VMEM((OUT, W), jnp.bfloat16),
            pltpu.VMEM((128, W), jnp.bfloat16),
            pltpu.SMEM((1,), jnp.int32),
            pltpu.SMEM((1,), jnp.int32),
            pltpu.SemaphoreType.DMA((OUT // 128,)),
        ] + [pltpu.SemaphoreType.DMA(())] * 3,
        compiler_params=pltpu.CompilerParams(vmem_limit_bytes=24 << 20),
    )(tab, cnt, rows_f, keys)


def plain_sort(keys_loc, rows_loc):
    sorted_keys, sort_order = lax.sort((keys_loc, lax.iota(jnp.int32, N)), num_keys=1)
    samples = sorted_keys[:: N // G]
    all_samples = jnp.sort(lax.all_gather(samples, "g", tiled=True))
    splitters = all_samples[G + G // 2 :: G]
    edges = jnp.searchsorted(sorted_keys, splitters, side="left").astype(jnp.int32)
    starts = jnp.concatenate([jnp.zeros((1,), jnp.int32), edges])
    stops = jnp.concatenate([edges, jnp.full((1,), N, jnp.int32)])
    src_pos = starts[:, None] + lax.iota(jnp.int32, CAP)[None, :]
    is_valid = src_pos < stops[:, None]
    src_pos = jnp.minimum(src_pos, N - 1)
    send_keys = jnp.where(is_valid, sorted_keys[src_pos], PAD_KEY)
    send_rows = jnp.where(is_valid[:, :, None], rows_loc[sort_order[src_pos]], 0.0)
    recv_keys = lax.all_to_all(send_keys, "g", 0, 0, tiled=True)
    recv_rows = lax.all_to_all(send_rows, "g", 0, 0, tiled=True)
    flat_keys = recv_keys.reshape(-1)
    merged_keys, merge_order = lax.sort((flat_keys, lax.iota(jnp.int32, OUT)), num_keys=1)
    return merged_keys, recv_rows.reshape(-1, W)[merge_order]


def solution(mesh):
    def local_part(keys_loc, rows_loc):
        rows_f, tab, keys_out, cnt = exchange(
            pltpu.with_memory_space_constraint(keys_loc.reshape(8, 128), pltpu.HBM),
            pltpu.with_memory_space_constraint(rows_loc, pltpu.HBM))
        rows_out, keys_out, count, flag = reorder(tab, cnt, rows_f, keys_out)

        def redo(state):
            keys_all, rows_all = plain_sort(keys_loc, rows_loc)
            return jnp.int32(0), keys_all, rows_all

        _, keys_sorted, rows_sorted = lax.while_loop(
            lambda state: state[0] > 0, redo, (flag.reshape(()), keys_out.reshape(-1), rows_out))
        return keys_sorted, rows_sorted, count

    row = P(("batch", "g"))
    mat = P(("batch", "g"), None)
    return jax.shard_map(local_part, mesh=mesh, in_specs=(row, mat), out_specs=(row, mat, row), check_vma=False)
```

```python
import functools
import jax
import jax.numpy as jnp
from jax import lax
from jax.sharding import PartitionSpec as P
from jax.experimental import pallas as pl
from jax.experimental.pallas import tpu as pltpu

PAD_KEY = 128.0
G = 128
N = 1024
W = 896
T = 7
CAP = 16
OUT = 2048
STRIDE = 11
CHIPS = G // 2
HOP = 29
PART = 8
LAG = 21
PER = 8
MESH = pl.DeviceIdType.MESH


def lane_iota(shape):
    return lax.broadcasted_iota(jnp.int32, shape, 1)


def sub_iota(shape):
    return lax.broadcasted_iota(jnp.int32, shape, 0)


def exchange_kernel(
    keys_hbm, pay_hbm, rows_f, tab_ref, keys_out, cnt_ref,
    keys_v, pay_b, pay_f, stage, sendbuf, recv, extra, samp, runs, kbuf, rk, srt, tab_v, st_v, tab_s, st_s,
    key_sem, in_sem, tab_sem, self_sem, s_send, s_recv, k_send, k_recv, p_send, f_send, p_recv, e_recv, f_recv,
):
    me = lax.axis_index("g")
    barrier = pltpu.get_barrier_semaphore()

    def peer(k):
        return (me + k * STRIDE) & (G - 1)

    core = me & 1
    chip = me // 2
    mate = me + 1 - 2 * core

    def ahead(k):
        return (chip + k * HOP) & (CHIPS - 1)

    def behind(k):
        return (chip - k * HOP) & (CHIPS - 1)

    def greet(k, c):
        pl.semaphore_signal(barrier, inc=1, device_id={"g": peer(k)}, device_id_type=MESH)
        return c

    key_load = pltpu.make_async_copy(keys_hbm, keys_v, key_sem)
    key_load.start()
    load = pltpu.make_async_copy(pay_hbm, pay_b, in_sem)
    load.start()
    lax.fori_loop(1, G, greet, 0)
    key_load.wait()

    keys = keys_v[...]
    keys_t = jnp.transpose(keys)
    rank_cols = []
    for a in range(8):
        col = keys_t[:, a : a + 1]
        acc = jnp.zeros((G, 128), jnp.int32)
        for b in range(8):
            acc = acc + (keys[b : b + 1, :] < col).astype(jnp.int32)
        rank_cols.append(jnp.sum(acc, axis=1, keepdims=True))
    def sort_row(r):
        want = lane_iota((G, 128)) * 8 + r
        ks = jnp.zeros((G, 128), jnp.float32)
        ps = jnp.zeros((G, 128), jnp.int32)
        for a in range(8):
            hit = rank_cols[a] == want
            src = sub_iota((G, 1)) + a * 128
            addr = (src >> 3) * (8 * T) + (src & 7)
            ks = ks + jnp.where(hit, keys_t[:, a : a + 1], 0.0)
            ps = ps + jnp.where(hit, addr, 0)
        row = jnp.sum(ks, axis=0, keepdims=True)
        srt[r : r + 1, :] = row
        tab_v[r : r + 1, :] = jnp.sum(ps, axis=0, keepdims=True)
        return row

    samp[...] = sort_row(0)
    pl.semaphore_wait(barrier, G - 1)

    def send_samples(k, c):
        pltpu.make_async_remote_copy(
            src_ref=samp, dst_ref=runs.at[pl.ds(me, 1), :], send_sem=s_send, recv_sem=s_recv,
            device_id={"g": peer(k)}, device_id_type=MESH,
        ).start()
        return c

    lax.fori_loop(1, G, send_samples, 0)

    for r in range(1, 8):
        sort_row(r)
    tab_copy = pltpu.make_async_copy(tab_v, tab_s, tab_sem)
    tab_copy.start()
    load.wait()

    def widen_rows(g, c):
        x = pay_b[pl.ds(pl.multiple_of(g * 16, 16), 16), :].astype(jnp.float32)
        base = pl.multiple_of(g * (16 * T), 16)
        for h in range(2):
            for t in range(T):
                pay_f[pl.ds(base + h * 8 * T + t * 8, 8), :] = x[h * 8 : h * 8 + 8, t * 128 : t * 128 + 128]
        return c

    lax.fori_loop(0, N // 16, widen_rows, 0)
    tab_copy.wait()

    many = runs.at[pl.ds(0, G - 1), :]
    pltpu.make_async_copy(many, many, s_recv).wait()
    pltpu.make_async_copy(many, many, s_send).wait()
    runs[pl.ds(me, 1), :] = samp[...]

    def reach(q_col):
        q = jnp.broadcast_to(q_col, (G, 128))

        def step(i, acc):
            for u in range(8):
                acc = acc + (runs[pl.ds(i * 8 + u, 1), :] <= q).astype(jnp.int32)
            return acc

        return jnp.sum(lax.fori_loop(0, G // 8, step, jnp.zeros((G, 128), jnp.int32)), axis=1, keepdims=True)

    sorted8 = srt[...]
    sorted8_t = jnp.transpose(sorted8)
    lanes = lane_iota((G, 128))
    need_row = jnp.where(lanes == 0, 0, lanes * 128 + 65)
    below = (reach(sorted8_t[:, 0:1]) < need_row).astype(jnp.int32)
    n_row = jnp.sum(below, axis=0, keepdims=True)
    at = jnp.broadcast_to(jnp.maximum(n_row - 1, 0), (8, 128))
    near = jnp.take_along_axis(sorted8, at, axis=1)
    near_t = jnp.transpose(near)
    n_t = jnp.transpose(jnp.broadcast_to(n_row, (8, 128)))[:, 0:1]
    dests = lax.broadcasted_iota(jnp.int32, (G, 1), 0)
    need = jnp.where(dests == 0, 0, dests * 128 + 65)
    pos = jnp.zeros((G, 1), jnp.int32)
    for width in (4, 2, 1):
        q = jnp.zeros((G, 1), jnp.float32)
        for j in range(width, 8, 2 * width):
            q = jnp.where(pos + width == j, near_t[:, j : j + 1], q)
        pos = pos + jnp.where(reach(q) < need, width, 0)
    start_col = jnp.where(n_t > 0, (n_t - 1) * 8 + pos + 1, 0)
    start = jnp.transpose(jnp.broadcast_to(start_col, (G, 128)))[0:1, :]
    stop = jnp.where(lanes[0:1, :] == G - 1, N, pltpu.roll(start, G - 1, 1))
    over = jnp.maximum(stop - start - PART, 0)
    odd = (lanes[0:1, :] & 1) == 1
    shift = jnp.where(odd, pltpu.roll(over, 1, 1), 0)
    full = jnp.where(odd & (over + shift > PART), 1, 0)
    full = jnp.max(full, axis=1, keepdims=True).astype(jnp.float32)
    shift_col = jnp.transpose(jnp.broadcast_to(shift, (8, 128)))[:, 0:1].astype(jnp.float32)
    st_v[...] = jnp.concatenate([start, over, jnp.zeros((6, 128), jnp.int32)], axis=0)
    st_copy = pltpu.make_async_copy(st_v, st_s, tab_sem)
    st_copy.start()

    st_copy.wait()

    def row_at(pos):
        pos = jnp.minimum(pos, N - 1)
        return pay_f[pl.ds(tab_s[pos & 7, pos >> 3], T, stride=8), :]

    def build(j):
        first = st_s[0, 2 * j]
        second = st_s[0, 2 * j + 1]
        split = st_s[1, 2 * j]
        for t in range(PART):
            stage[pl.ds(t, T, stride=8), :] = row_at(first + t)
            stage[pl.ds(8 * T + t, T, stride=8), :] = row_at(second + t)
            stage[pl.ds(16 * T + t, T, stride=8), :] = row_at(
                jnp.where(t < split, first + PART + t, second + PART + t - split))
        for h in range(3):
            for c in range(T):
                base = h * 8 * T + c * 8
                sendbuf[j * 3 + h, :, c * 128 : c * 128 + 128] = stage[base : base + 8, :].astype(jnp.bfloat16)

    def send_part(src, dst, to, sem):
        pltpu.make_async_remote_copy(
            src_ref=src, dst_ref=dst.at[me], send_sem=p_send, recv_sem=sem,
            device_id={"g": to}, device_id_type=MESH,
        ).start()

    def send_c(k):
        j = ahead(k)
        build(j)
        send_part(sendbuf.at[j * 3 + 2], extra, 2 * j + core, e_recv.at[k])

    def send_a(k):
        j = ahead(k)
        send_part(sendbuf.at[j * 3], recv, 2 * j, p_recv.at[k // PER])

    def send_b(k):
        j = ahead(k)
        send_part(sendbuf.at[j * 3 + 1], recv, 2 * j + 1, p_recv.at[k // PER])

    def send_keys(k):
        p = peer(k)
        pltpu.make_async_remote_copy(
            src_ref=kbuf.at[pl.ds(p, 1), :], dst_ref=rk.at[pl.ds(me, 1), :], send_sem=k_send, recv_sem=k_recv,
            device_id={"g": p}, device_id_type=MESH,
        ).start()

    def key_steps(k, c):
        send_c(k)
        send_a(k - LAG)
        for u in range(8):
            i = (k - LAG) * 8 + u - 7

            @pl.when(i < G)
            def _():
                send_keys(i)
        return c

    def steps(lo, hi, what):
        def step(k, c):
            if "c" in what:
                send_c(k)
            if "a" in what:
                send_a(k - LAG)
            if "b" in what:
                send_b(k - 2 * LAG)
            return c

        lax.fori_loop(lo, hi, step, 0)

    steps(1, LAG + 1, "c")

    stop_col = jnp.transpose(jnp.broadcast_to(stop, (8, 128)))[:, 0:1]
    tables = [jnp.broadcast_to(sorted8[b : b + 1, :], (8, 128)) for b in range(8)]
    for dg in range(16):
        first = start_col[dg * 8 : dg * 8 + 8, :]
        last = stop_col[dg * 8 : dg * 8 + 8, :]
        slot = lane_iota((8, 128))
        idx = first + slot
        pick = (idx >> 3) & 127
        part = idx & 7
        val = jnp.full((8, 128), PAD_KEY, jnp.float32)
        for b in range(8):
            val = jnp.where(part == b, jnp.take_along_axis(tables[b], pick, axis=1), val)
        val = jnp.where((idx < last) & (slot < CAP), val, PAD_KEY)
        val = jnp.where(slot == CAP, shift_col[dg * 8 : dg * 8 + 8, :], val)
        kbuf[dg * 8 : dg * 8 + 8, :] = jnp.where(slot == CAP + 1, full, val)

    lax.fori_loop(LAG + 1, LAG + 1 + G // 8, key_steps, 0)
    steps(LAG + 1 + G // 8, 2 * LAG + 1, "ca")
    steps(2 * LAG + 1, CHIPS, "cab")
    steps(CHIPS, CHIPS + LAG, "ab")
    steps(CHIPS + LAG, CHIPS + 2 * LAG, "b")
    build(chip)
    send_part(sendbuf.at[chip * 3 + 1 - core], recv, mate, p_recv.at[0])
    send_part(sendbuf.at[chip * 3 + 2], extra, mate, f_recv.at[0])
    own = pltpu.make_async_copy(sendbuf.at[chip * 3 + core], recv.at[me], self_sem)
    own.start()
    own_extra = pltpu.make_async_copy(sendbuf.at[chip * 3 + 2], extra.at[me], key_sem)
    own_extra.start()

    many_k = rk.at[pl.ds(0, G - 1), :]
    pltpu.make_async_copy(many_k, many_k, k_recv).wait()
    pltpu.make_async_copy(many_k, many_k, k_send).wait()
    rk[pl.ds(me, 1), :] = kbuf[pl.ds(me, 1), :]
    got = rk[...]
    kt = jnp.transpose(got)[0:CAP, :]
    valid = (kt < PAD_KEY).astype(jnp.int32)
    n_valid = jnp.sum(jnp.sum(valid, axis=1, keepdims=True), axis=0, keepdims=True)
    any_full = jnp.max(got[:, CAP + 1 : CAP + 2], axis=0, keepdims=True).astype(jnp.int32)
    cnt_ref[...] = jnp.where(lanes[0:1, :] == 0, n_valid, any_full)
    skip = got[:, CAP : CAP + 1].astype(jnp.int32)
    cols = []
    for t in range(CAP):
        col = got[:, t : t + 1]
        acc = jnp.zeros((G, 128), jnp.int32)
        for u in range(CAP):
            acc = acc + (kt[u : u + 1, :] < col).astype(jnp.int32)
        cols.append(jnp.sum(acc, axis=1, keepdims=True))
    places = []
    for r in range(OUT // 128):
        want = lane_iota((G, 128)) + r * 128
        wish = lane_iota((G, 128)) * 16 + r
        ks = jnp.zeros((G, 128), jnp.float32)
        ps = jnp.zeros((G, 128), jnp.int32)
        for t in range(CAP):
            if t < PART:
                addr = sub_iota((G, 1)) * (8 * T) + t
            else:
                addr = (sub_iota((G, 1)) + G) * (8 * T) + jnp.minimum(skip + (t - PART), PART - 1)
            ks = ks + jnp.where(cols[t] == want, got[:, t : t + 1], 0.0)
            ps = ps + jnp.where(cols[t] == wish, addr, 0)
        live = want[0:1, :] < n_valid
        keys_out[r : r + 1, :] = jnp.where(live, jnp.sum(ks, axis=0, keepdims=True), PAD_KEY)
        places.append(jnp.where(wish[0:1, :] < n_valid, jnp.sum(ps, axis=0, keepdims=True), OUT * T))
    tab_ref[...] = jnp.transpose(jnp.concatenate(places, axis=0))
    rows_f[pl.ds(OUT * T, 8 * T), :] = jnp.zeros((8 * T, 128), jnp.float32)

    def widen(part, src, first):
        x = part[src].astype(jnp.float32)
        base = pl.multiple_of((first + src) * (8 * T), 8)
        for t in range(T):
            rows_f[pl.ds(base + t * 8, 8), :] = x[:, t * 128 : t * 128 + 128]

    own.wait()
    own_extra.wait()
    widen(recv, me, 0)
    widen(extra, me, G)
    one = extra.at[0]

    def forward(k, c):
        pltpu.make_async_copy(one, one, e_recv.at[k]).wait()
        src = 2 * behind(k) + core
        pltpu.make_async_remote_copy(
            src_ref=extra.at[src], dst_ref=extra.at[src], send_sem=f_send, recv_sem=f_recv.at[k // PER],
            device_id={"g": mate}, device_id_type=MESH,
        ).start()
        return c

    def widen_direct(k, c):
        j = behind(k)
        widen(recv, 2 * j, 0)
        widen(recv, 2 * j + 1, 0)
        widen(extra, 2 * j + core, G)
        return c

    def widen_forwarded(k, c):
        widen(extra, 2 * behind(k) + 1 - core, G)
        return c

    for g in range(CHIPS // PER):
        lo = max(1, g * PER)
        hi = (g + 1) * PER
        lax.fori_loop(lo, hi, forward, 0)
        got_part = recv.at[pl.ds(0, 2 * PER - 1 if g == 0 else 2 * PER)]
        pltpu.make_async_copy(got_part, got_part, p_recv.at[g]).wait()
        if g == 0:
            widen(recv, mate, 0)
        lax.fori_loop(lo, hi, widen_direct, 0)
        if g > 0:
            fw = extra.at[pl.ds(0, PER)]
            pltpu.make_async_copy(fw, fw, f_recv.at[g - 1]).wait()
            lax.fori_loop((g - 1) * PER, g * PER, widen_forwarded, 0)
    fw = extra.at[pl.ds(0, PER)]
    pltpu.make_async_copy(fw, fw, f_recv.at[CHIPS // PER - 1]).wait()
    lax.fori_loop(CHIPS - PER, CHIPS, widen_forwarded, 0)
    sent = sendbuf.at[pl.ds(0, 3 * (CHIPS - 1) + 2)]
    pltpu.make_async_copy(sent, sent, p_send).wait()
    passed = extra.at[pl.ds(0, CHIPS - 1)]
    pltpu.make_async_copy(passed, passed, f_send).wait()


def exchange(keys8, rows):
    vmem = pl.BlockSpec(memory_space=pltpu.VMEM)
    hbm = pl.BlockSpec(memory_space=pltpu.HBM)
    return pl.pallas_call(
        exchange_kernel,
        out_shape=(
            jax.ShapeDtypeStruct(((OUT + 8) * T + 8, 128), jnp.float32),
            jax.ShapeDtypeStruct((G, 16), jnp.int32),
            jax.ShapeDtypeStruct((OUT // 128, 128), jnp.float32),
            jax.ShapeDtypeStruct((1, 128), jnp.int32),
        ),
        in_specs=[hbm, hbm],
        out_specs=(vmem, vmem, vmem, vmem),
        scratch_shapes=[
            pltpu.VMEM((8, 128), jnp.float32),
            pltpu.VMEM((N, W), jnp.bfloat16),
            pltpu.VMEM((N * T + 8, 128), jnp.float32),
            pltpu.VMEM((24 * T + 8, 128), jnp.float32),
            pltpu.VMEM((3 * CHIPS, PART, W), jnp.bfloat16),
            pltpu.VMEM((G, PART, W), jnp.bfloat16),
            pltpu.VMEM((G, PART, W), jnp.bfloat16),
            pltpu.VMEM((1, 128), jnp.float32),
            pltpu.VMEM((G, 128), jnp.float32),
            pltpu.VMEM((G, 128), jnp.float32),
            pltpu.VMEM((G, 128), jnp.float32),
            pltpu.VMEM((8, 128), jnp.float32),
            pltpu.VMEM((8, 128), jnp.int32),
            pltpu.VMEM((8, 128), jnp.int32),
            pltpu.SMEM((8, 128), jnp.int32),
            pltpu.SMEM((8, 128), jnp.int32),
        ] + [pltpu.SemaphoreType.DMA(())] * 10 + [
            pltpu.SemaphoreType.DMA((CHIPS // PER,)),
            pltpu.SemaphoreType.DMA((CHIPS,)),
            pltpu.SemaphoreType.DMA((CHIPS // PER,)),
        ],
        compiler_params=pltpu.CompilerParams(
            collective_id=1, has_side_effects=True, vmem_limit_bytes=40 << 20),
    )(keys8, rows)


def order_kernel(tab_s, cnt_s, rows_f, keys_v, pay_hbm, keys_hbm, cnt_hbm, flag_hbm, stage, outb, zeros, cnt_v, flag_v, out_sem, key_sem, cnt_sem, flag_sem):
    count = cnt_s[0, 0]
    cnt_v[0] = count
    flag_v[0] = cnt_s[0, 1]
    cnt_store = pltpu.make_async_copy(cnt_v, cnt_hbm, cnt_sem)
    cnt_store.start()
    flag_store = pltpu.make_async_copy(flag_v, flag_hbm, flag_sem)
    flag_store.start()
    keys_store = pltpu.make_async_copy(keys_v, keys_hbm, key_sem)
    keys_store.start()
    rows = 128
    chunks = OUT // rows
    zeros[...] = jnp.zeros((rows, W), jnp.bfloat16)

    def store(i, src):
        return pltpu.make_async_copy(
            src, pay_hbm.at[pl.ds(pl.multiple_of(i * rows, rows), rows), :], out_sem.at[i])

    def place(g, c):
        for t in range(16):
            addr = tab_s[g, t]
            stage[pl.ds((t // 8) * 8 * T + (t % 8), T, stride=8), :] = rows_f[pl.ds(addr, T, stride=8), :]
        for q in range(T):
            block = jnp.concatenate(
                [stage[q * 8 : q * 8 + 8, :], stage[8 * T + q * 8 : 8 * T + q * 8 + 8, :]], axis=0)
            outb[pl.ds(pl.multiple_of(g * 16, 16), 16), q * 128 : q * 128 + 128] = block.astype(jnp.bfloat16)
        return c

    def empty(i, c):
        @pl.when(i * rows >= count)
        def _():
            store(i, zeros).start()
        return c

    def full(i, c):
        @pl.when(i * rows < count)
        def _():
            lax.fori_loop(i * (rows // 16), (i + 1) * (rows // 16), place, 0)
            store(i, outb.at[pl.ds(pl.multiple_of(i * rows, rows), rows), :]).start()
        return c

    def finish(i, c):
        store(i, zeros).wait()
        return c

    lax.fori_loop(0, chunks, empty, 0)
    lax.fori_loop(0, chunks, full, 0)
    keys_store.wait()
    cnt_store.wait()
    flag_store.wait()
    lax.fori_loop(0, chunks, finish, 0)


def reorder(tab, cnt, rows_f, keys):
    smem = pl.BlockSpec(memory_space=pltpu.SMEM)
    vmem = pl.BlockSpec(memory_space=pltpu.VMEM)
    hbm = pl.BlockSpec(memory_space=pltpu.HBM)
    return pl.pallas_call(
        order_kernel,
        out_shape=(
            jax.ShapeDtypeStruct((OUT, W), jnp.bfloat16),
            jax.ShapeDtypeStruct((OUT // 128, 128), jnp.float32),
            jax.ShapeDtypeStruct((1,), jnp.int32),
            jax.ShapeDtypeStruct((1,), jnp.int32),
        ),
        in_specs=[smem, smem, vmem, vmem],
        out_specs=(hbm, hbm, hbm, hbm),
        scratch_shapes=[
            pltpu.VMEM((16 * T + 8, 128), jnp.float32),
            pltpu.VMEM((OUT, W), jnp.bfloat16),
            pltpu.VMEM((128, W), jnp.bfloat16),
            pltpu.SMEM((1,), jnp.int32),
            pltpu.SMEM((1,), jnp.int32),
            pltpu.SemaphoreType.DMA((OUT // 128,)),
        ] + [pltpu.SemaphoreType.DMA(())] * 3,
        compiler_params=pltpu.CompilerParams(vmem_limit_bytes=24 << 20),
    )(tab, cnt, rows_f, keys)


def plain_sort(keys_loc, rows_loc):
    sorted_keys, sort_order = lax.sort((keys_loc, lax.iota(jnp.int32, N)), num_keys=1)
    samples = sorted_keys[:: N // G]
    all_samples = jnp.sort(lax.all_gather(samples, "g", tiled=True))
    splitters = all_samples[G + G // 2 :: G]
    edges = jnp.searchsorted(sorted_keys, splitters, side="left").astype(jnp.int32)
    starts = jnp.concatenate([jnp.zeros((1,), jnp.int32), edges])
    stops = jnp.concatenate([edges, jnp.full((1,), N, jnp.int32)])
    src_pos = starts[:, None] + lax.iota(jnp.int32, CAP)[None, :]
    is_valid = src_pos < stops[:, None]
    src_pos = jnp.minimum(src_pos, N - 1)
    send_keys = jnp.where(is_valid, sorted_keys[src_pos], PAD_KEY)
    send_rows = jnp.where(is_valid[:, :, None], rows_loc[sort_order[src_pos]], 0.0)
    recv_keys = lax.all_to_all(send_keys, "g", 0, 0, tiled=True)
    recv_rows = lax.all_to_all(send_rows, "g", 0, 0, tiled=True)
    flat_keys = recv_keys.reshape(-1)
    merged_keys, merge_order = lax.sort((flat_keys, lax.iota(jnp.int32, OUT)), num_keys=1)
    return merged_keys, recv_rows.reshape(-1, W)[merge_order]


def solution(mesh):
    def local_part(keys_loc, rows_loc):
        rows_f, tab, keys_out, cnt = exchange(
            pltpu.with_memory_space_constraint(keys_loc.reshape(8, 128), pltpu.HBM),
            pltpu.with_memory_space_constraint(rows_loc, pltpu.HBM))
        rows_out, keys_out, count, flag = reorder(tab, cnt, rows_f, keys_out)

        def redo(state):
            keys_all, rows_all = plain_sort(keys_loc, rows_loc)
            return jnp.int32(0), keys_all, rows_all

        _, keys_sorted, rows_sorted = lax.while_loop(
            lambda state: state[0] > 0, redo, (flag.reshape(()), keys_out.reshape(-1), rows_out))
        return keys_sorted, rows_sorted, count

    row = P(("batch", "g"))
    mat = P(("batch", "g"), None)
    return jax.shard_map(local_part, mesh=mesh, in_specs=(row, mat), out_specs=(row, mat, row), check_vma=False)
```
